128 devices in a mesh: section: 4 (over y_lo, core), tensor: 4 (over x), dp: 8 (over y_hi, z).
Axes of the slice: x: 4, y: 4 (y_hi: 2, y_lo: 2; y = y_hi * 2 + y_lo), z: 4, core: 2. Of those that a mesh axis runs over, the one named last changes fastest.
Arguments:
- layer_in: bfloat16 [2, 2, 4, 8, 128, 2560], P(None, None, 'section', 'dp', 'tensor'), may hold values from -6 to 6
- carry_in: bfloat16 [2, 4, 8, 128, 2560], P(None, 'section', 'dp', 'tensor'), may hold values from -6 to 6
- top_grad: bfloat16 [1, 8, 128, 2560], P(None, 'dp', 'tensor'), may hold values from -6 to 6
- w_qkv: bfloat16 [2, 4, 2560, 2560], P(None, 'section', None, 'tensor'), may hold values from -1 to 1
- w_out: bfloat16 [2, 4, 2048, 2560], P(None, 'section', 'tensor'), may hold values from -0.125 to 0.125
- gain: float32 [2, 4, 2560], P(None, 'section'), may hold values from 0.5 to 1.5
Outputs:
- unit_grads: bfloat16 [2, 2, 4, 8, 128, 2560], P(None, None, 'section', 'dp', 'tensor')
- grad_qkv: bfloat16 [2, 4, 2560, 2560], P(None, 'section', 'dp', 'tensor')
- grad_out: bfloat16 [2, 4, 2048, 2560], P(None, 'section', ('tensor', 'dp'))
- grad_gain: float32 [2, 4, 2560], P(None, 'section')
The draws below stay inside these ranges and needn't reach their ends.
All inputs are finite; a program needn't handle non-finite values.
Results may differ from the reference program's by a relative error of at most 0.022.
The reference program's roundings to bfloat16 on the way count: a program that leaves them out, or rounds other values in their place, can miss the bound.
Values may be sent and summed in bfloat16 or wider, within the bound.
A program may use at most 128 MiB of HBM per device.

```python
import math
import jax
import jax.numpy as jnp
from jax import lax

D = 2560
KV = 4
HD = 64
SEQ = 128
TICKS = 2
GROUP = 8
HQ = 2048
QKV = 2560
SECTIONS = 4
REPLICAS = 8
N_TENSOR = 4


def draw_w_qkv(key, part):
    draw_shape = (2, SECTIONS, D, KV, GROUP + 2, HD)
    entries = jax.random.normal(key, draw_shape, jnp.float32) / jnp.sqrt(jnp.float32(D))
    return jnp.clip(entries, -1.0, 1.0).reshape(2, SECTIONS, D, KV * (GROUP + 2) * HD).astype(jnp.bfloat16)


def level_of(stream_key, shape, pieces, smallest, largest):
    def one(axis_at, parts):
        steps = jax.random.uniform(jax.random.fold_in(jax.random.fold_in(stream_key, 6), axis_at), (parts,), jnp.float32, smallest / len(pieces), largest / len(pieces))
        return jnp.repeat(jnp.exp(steps), shape[axis_at] // parts).reshape((-1,) + (1,) * (len(shape) - axis_at - 1))

    factor_of = one(*pieces[0])
    for cut in pieces[1:]:
        factor_of = factor_of * one(*cut)
    return factor_of


def gaussian(own_key, extent, spread, most, cuts=(), kind=jnp.bfloat16):
    values = spread * jax.random.normal(own_key, extent, jnp.float32)
    if cuts:
        values = values * level_of(own_key, extent, cuts, -0.22, 0.18)
    return jnp.clip(values, -most, most).astype(kind)


def setup_inputs(seed: int = 0) -> dict:
    arg_keys = jax.random.split(jax.random.key(seed), 7)
    return {
        "layer_in": gaussian(arg_keys[0], (TICKS, 2, SECTIONS, REPLICAS, SEQ, D), 1.0, 6.0, ((2, 4), (3, 8), (4, 4))),
        "carry_in": gaussian(arg_keys[1], (2, SECTIONS, REPLICAS, SEQ, D), 1.0, 6.0, ((1, 4), (2, 8), (3, 4))),
        "top_grad": gaussian(arg_keys[2], (TICKS - 1, REPLICAS, SEQ, D), 1.0, 6.0, ((1, 8), (2, 4))),
        "w_qkv": draw_w_qkv(jax.random.fold_in(arg_keys[6], 71), 0),
        "w_out": gaussian(arg_keys[4], (2, SECTIONS, HQ, D), HQ ** -0.5, 0.125, ((1, 4), (2, 4))),
        "gain": jnp.clip(1.0 + 0.1 * jax.random.normal(arg_keys[5], (2, SECTIONS, D), jnp.float32), 0.5, 1.5),
    }


epsilon = 1e-06
rope_base = 1000000.0

def rope_tables(length, head_width):
    half_width = head_width // 2
    exponent = jnp.arange(half_width, dtype=jnp.float32) * (2.0 / head_width)
    frequency = rope_base ** (-exponent)
    angle = jnp.arange(length, dtype=jnp.float32)[:, None] * frequency[None, :]
    return (jnp.cos(angle), jnp.sin(angle))

def rotate(values, cosine_table, sine_table, direction):
    half_width = values.shape[-1] // 2
    table_shape = (values.shape[0],) + (1,) * (values.ndim - 2) + (half_width,)
    cosine = cosine_table.reshape(table_shape)
    sine_part = direction * sine_table.reshape(table_shape)
    lower_half = values[..., :half_width]
    upper_half = values[..., half_width:]
    return jnp.concatenate([lower_half * cosine - upper_half * sine_part, upper_half * cosine + lower_half * sine_part], axis=-1)

def layer_backward(layer_rows, grad_output, weight_qkv, weight_out, gain_row):
    length = layer_rows.shape[0]
    cosine_table, sine_table = rope_tables(length, HD)
    inputs_float = layer_rows.astype(jnp.float32)
    inverse = lax.rsqrt(lax.optimization_barrier(jnp.mean(inputs_float * inputs_float, axis=-1, keepdims=True)) + epsilon)
    unit_rows = inputs_float * inverse
    normed = (unit_rows * gain_row).astype(jnp.bfloat16)
    projected = jnp.dot(normed, weight_qkv, preferred_element_type=jnp.float32).reshape(length, KV, GROUP + 2, HD)
    query_rot = rotate(projected[:, :, :GROUP], cosine_table, sine_table, 1.0).astype(jnp.bfloat16)
    key_rot = rotate(projected[:, :, GROUP], cosine_table, sine_table, 1.0).astype(jnp.bfloat16)
    value_rows = projected[:, :, GROUP + 1].astype(jnp.bfloat16)
    query_float = query_rot.astype(jnp.float32)
    key_float = key_rot.astype(jnp.float32)
    value_float = value_rows.astype(jnp.float32)
    score_scale = 1.0 / math.sqrt(HD)
    scores = jnp.einsum('tkgd,ukd->kgtu', query_float, key_float) * score_scale
    causal_mask = jnp.arange(length)[:, None] >= jnp.arange(length)[None, :]
    scores = jnp.where(causal_mask, scores, -1e+30)
    exponentials = jnp.exp(scores - lax.optimization_barrier(jnp.max(scores, axis=-1, keepdims=True)))
    softmax_rows = exponentials / lax.optimization_barrier(jnp.sum(exponentials, axis=-1, keepdims=True))
    softmax_low = softmax_rows.astype(jnp.bfloat16)
    softmax_float = softmax_low.astype(jnp.float32)
    attended = jnp.einsum('kgtu,ukd->tkgd', softmax_float, value_float).astype(jnp.bfloat16).reshape(length, HQ)
    grad_attended = jnp.dot(grad_output, weight_out.T, preferred_element_type=jnp.float32).astype(jnp.bfloat16)
    grad_heads = grad_attended.reshape(length, KV, GROUP, HD).astype(jnp.float32)
    grad_softmax = jnp.einsum('tkgd,ukd->kgtu', grad_heads, value_float)
    row_total = lax.optimization_barrier(jnp.sum(softmax_rows * grad_softmax, axis=-1, keepdims=True))
    grad_scores = (softmax_rows * (grad_softmax - row_total) * score_scale).astype(jnp.bfloat16)
    grad_score_float = grad_scores.astype(jnp.float32)
    grad_value = jnp.einsum('kgtu,tkgd->ukd', softmax_float, grad_heads)
    grad_query = rotate(jnp.einsum('kgtu,ukd->tkgd', grad_score_float, key_float), cosine_table, sine_table, -1.0)
    grad_key = rotate(jnp.einsum('kgtu,tkgd->ukd', grad_score_float, query_float), cosine_table, sine_table, -1.0)
    grad_projected = jnp.concatenate([grad_query, grad_key[:, :, None], grad_value[:, :, None]], axis=2)
    grad_projected = grad_projected.reshape(length, QKV).astype(jnp.bfloat16)
    block_width = QKV // N_TENSOR
    grad_normed = jnp.zeros((length, D), jnp.float32)
    for column_block in range(N_TENSOR):
        lower = column_block * block_width
        block_term = jnp.dot(grad_projected[:, lower:lower + block_width], weight_qkv[:, lower:lower + block_width].T, preferred_element_type=jnp.float32)
        grad_normed = grad_normed + block_term.astype(jnp.bfloat16).astype(jnp.float32)
    grad_unit = grad_normed * gain_row
    grad_rows = inverse * (grad_unit - unit_rows * lax.optimization_barrier(jnp.mean(grad_unit * unit_rows, axis=-1, keepdims=True)))
    grad_input = (grad_output.astype(jnp.float32) + grad_rows).astype(jnp.bfloat16)
    grad_scale = lax.optimization_barrier(jnp.sum(grad_normed * unit_rows, axis=0))
    grad_wqkv = jnp.dot(normed.T, grad_projected, preferred_element_type=jnp.float32)
    grad_wout = jnp.dot(attended.T, grad_output, preferred_element_type=jnp.float32)
    return (grad_input, grad_wqkv, grad_wout, grad_scale)

def reference(layer_in, carry_in, top_grad, w_qkv, w_out, gain):
    ticks = layer_in.shape[0]
    sections = layer_in.shape[2]
    per_replica = (jnp.moveaxis(layer_in, 3, 0), jnp.moveaxis(carry_in, 2, 0), jnp.moveaxis(top_grad, 1, 0))

    def one_replica(totals, slices):
        layer_rows, carried, fresh_grads = slices
        sum_qkv = jnp.zeros(w_qkv.shape, jnp.float32)
        sum_out = jnp.zeros(w_out.shape, jnp.float32)
        gain_total = totals[2]
        produced = {}
        per_tick = []
        for position in range(ticks):
            current = {}
            for member in (1, 0):
                for section_index in range(sections):
                    if position == 0:
                        incoming = carried[member, section_index]
                    elif member == 1 and section_index == 0:
                        incoming = fresh_grads[position - 1]
                    elif member == 1:
                        incoming = produced[1, section_index - 1]
                    elif section_index == sections - 1:
                        incoming = produced[1, section_index]
                    else:
                        incoming = produced[0, section_index + 1]
                    outcome = layer_backward(layer_rows[position, member, section_index], incoming, w_qkv[member, section_index], w_out[member, section_index], gain[member, section_index])
                    current[member, section_index] = outcome[0]
                    sum_qkv = sum_qkv.at[member, section_index].add(outcome[1])
                    sum_out = sum_out.at[member, section_index].add(outcome[2])
                    gain_total = gain_total.at[member, section_index].add(outcome[3])
            produced = current
            per_tick.append(jnp.stack([jnp.stack([current[member, index] for index in range(sections)]) for member in (0, 1)]))
        new_qkv = totals[0] + sum_qkv.astype(jnp.bfloat16).astype(jnp.float32)
        new_out = totals[1] + sum_out.astype(jnp.bfloat16).astype(jnp.float32)
        return ((new_qkv, new_out, gain_total), jnp.stack(per_tick))
    start_totals = (jnp.zeros(w_qkv.shape, jnp.float32), jnp.zeros(w_out.shape, jnp.float32), jnp.zeros(gain.shape, jnp.float32))
    totals, grads_all = lax.scan(one_replica, start_totals, per_replica)
    unit_grads = jnp.moveaxis(grads_all, 0, 3)
    return (unit_grads, totals[0].astype(jnp.bfloat16), totals[1].astype(jnp.bfloat16), totals[2])
```

```python
import functools
import math

import jax
import jax.numpy as jnp
from jax import lax
from jax.experimental import pallas as pl
from jax.experimental.pallas import tpu as pltpu
from jax.sharding import PartitionSpec as P

HD = 64
GROUP = 8
EPSILON = 1e-06
ROPE_BASE = 1000000.0
SCALE = 1.0 / math.sqrt(HD)
F32 = jnp.float32
BF16 = jnp.bfloat16
MESH = pl.DeviceIdType.MESH
DIMS = dict(ticks=2, sections=4, tensor=4, dp=8)


def rope_tables(length):
    half = HD // 2
    exponent = jnp.arange(half, dtype=F32) * (2.0 / HD)
    frequency = ROPE_BASE ** (-exponent)
    angle = jnp.arange(length, dtype=F32)[:, None] * frequency[None, :]
    cosine, sine = jnp.cos(angle), jnp.sin(angle)
    head_cos = jnp.concatenate([cosine, cosine], axis=1)
    head_sin = jnp.concatenate([-sine, sine], axis=1)
    return jnp.stack(
        [
            jnp.concatenate([head_cos, head_cos], axis=1),
            jnp.concatenate([head_sin, head_sin], axis=1),
            jnp.concatenate([head_cos, jnp.ones_like(head_cos)], axis=1),
            jnp.concatenate([head_sin, jnp.zeros_like(head_sin)], axis=1),
        ]
    )


def nt(a, b):
    return lax.dot_general(a, b, (((1,), (1,)), ((), ())), preferred_element_type=F32)


def tn(a, b):
    return lax.dot_general(a, b, (((0,), (0,)), ((), ())), preferred_element_type=F32)


def nn(a, b):
    return jnp.dot(a, b, preferred_element_type=F32)


def kernel(
    x_hbm, c_hbm, t_hbm, wq_hbm, wo_hbm, gain_hbm, rope_hbm,
    ug_out, gq_out, go_out, gg_out,
    wq, wo, gain, rope, xg, dyg, n_t, n_tr, gpr, q_rot, kk, vv, prob, att, gn, rsr, ug,
    part, part_r, gain_sum, g1, g2, gq_v, go_v, gg_v,
    w_sem, own_sem, out_sem, ag_s, ag_r, dy_s, dy_r, rs_s, rs_r, sh_s, sh_r,
    nt_s, nt_r, gp_s, gp_r, po_s, po_r, g1_s, g1_r, g2_s, g2_r,
):
    s, c, j = lax.axis_index("section"), lax.axis_index("tensor"), lax.axis_index("dp")
    n_s, n_c, n_j = DIMS["sections"], DIMS["tensor"], DIMS["dp"]
    rows = x_hbm.shape[1]
    length = rows * n_c
    width = x_hbm.shape[2]
    slice_q = gq_out.shape[1]
    slice_o = go_out.shape[1]
    own = pl.ds(pl.multiple_of(c * rows, rows), rows)
    lane = lax.broadcasted_iota(jnp.int32, (length, 128), 1)
    low_half = (lane % HD) < (HD // 2)
    first_head = lane < HD

    def tensor_peer(k):
        return lax.rem(c + k, n_c)

    def dp_peer(k):
        z, y = lax.rem(j, 4), lax.div(j, 4)
        return lax.rem(y + k // 4, 2) * 4 + lax.rem(z + k % 4, 4)

    sent = []

    def send(src, dst, s_sem, r_sem, to):
        copy = pltpu.make_async_remote_copy(
            src_ref=src, dst_ref=dst, send_sem=s_sem, recv_sem=r_sem, device_id=to, device_id_type=MESH
        )
        copy.start()
        sent.append(copy)
        return copy

    loads = {}

    def load(name, src, dst, i):
        loads[name] = pltpu.make_async_copy(src, dst, w_sem.at[i])
        loads[name].start()

    load("gain", gain_hbm, gain, 0)
    load("rope", rope_hbm, rope, 1)
    own_copies = {}
    for i, (name, src, dst) in enumerate(
        [(("x", u), x_hbm.at[u], xg.at[u, own]) for u in range(4)]
        + [(("d", u), c_hbm.at[u], dyg.at[u, own]) for u in range(2)]
    ):
        own_copies[name] = pltpu.make_async_copy(src, dst, own_sem.at[i])
        own_copies[name].start()
    load("wq1", wq_hbm.at[1], wq.at[1], 2)
    load("wo1", wo_hbm.at[1], wo.at[1], 3)
    load("wq0", wq_hbm.at[0], wq.at[0], 4)
    load("wo0", wo_hbm.at[0], wo.at[0], 5)

    gathers = {}

    def gather_x(u):
        gathers["x", u] = [
            send(x_hbm.at[u], xg.at[u, own], ag_s.at[u, k - 1], ag_r.at[u, k - 1], (s, tensor_peer(k), j))
            for k in (1, 3, 2)
        ]

    def gather_d(u):
        src = c_hbm.at[u] if u < 2 else dyg.at[u, own]
        gathers["d", u] = [
            send(src, dyg.at[u, own], dy_s.at[u, k - 1], dy_r.at[u, k - 1], (s, tensor_peer(k), j))
            for k in (1, 3, 2)
        ]

    def gathered(kind, u):
        if (kind, u) in own_copies:
            own_copies[kind, u].wait()
        for copy in gathers[kind, u]:
            copy.wait_recv()

    def partner(chunk):
        return jnp.where(low_half, pltpu.roll(chunk, 96, 1), pltpu.roll(chunk, 32, 1))

    def forward(u):
        t, m = u // 2, u % 2
        x = xg[u].astype(F32)
        inverse = lax.rsqrt(jnp.mean(x * x, axis=-1, keepdims=True) + EPSILON)
        normed = (x * inverse * gain[m : m + 1, :]).astype(BF16)
        for i in range(width // 256):
            n_t[u, i * 256 : (i + 1) * 256, :] = jnp.transpose(normed[:, i * 256 : (i + 1) * 256])
        projected = nn(normed, wq[m])
        for i in range(4):
            chunk = projected[:, i * 128 : (i + 1) * 128]
            q_rot[u, :, i * 128 : (i + 1) * 128] = (chunk * rope[0] + partner(chunk) * rope[1]).astype(BF16)
        chunk = projected[:, 512:640]
        both = (chunk * rope[2] + partner(chunk) * rope[3]).astype(BF16).astype(F32)
        key_low = jnp.where(first_head, both, 0.0)
        value_high = jnp.where(first_head, 0.0, both)
        kk[u, 0:128, :] = key_low.astype(BF16)
        kk[u, 128:256, :] = pltpu.roll(key_low, HD, 1).astype(BF16)
        vv[u, 0:128, :] = pltpu.roll(value_high, HD, 1).astype(BF16)
        vv[u, 128:256, :] = value_high.astype(BF16)
        causal = lax.broadcasted_iota(jnp.int32, (length, length), 0) >= lax.broadcasted_iota(
            jnp.int32, (length, length), 1
        )
        for i in range(4):
            scores = nt(q_rot[u, :, i * 128 : (i + 1) * 128], kk[u]) * SCALE
            low = []
            for h in range(2):
                part_scores = jnp.where(causal, scores[:, h * 128 : (h + 1) * 128], -1e30)
                e = jnp.exp(part_scores - jnp.max(part_scores, axis=-1, keepdims=True))
                p = e / jnp.sum(e, axis=-1, keepdims=True)
                prob[u, :, (2 * i + h) * 128 : (2 * i + h + 1) * 128] = p
                low.append(p.astype(BF16))
            att[m, t * 128 : (t + 1) * 128, i * 128 : (i + 1) * 128] = nn(
                jnp.concatenate(low, axis=1), vv[u]
            ).astype(BF16)

    def backward(u):
        t, m = u // 2, u % 2
        grad_att = nt(dyg[u], wo[m]).astype(BF16)
        acc_k = jnp.zeros((256, 128), F32)
        acc_v = jnp.zeros((256, 128), F32)
        slot = pl.ds(pl.multiple_of((j * 2 + t) * 128, 128), 128)
        for i in range(4):
            da = grad_att[:, i * 128 : (i + 1) * 128]
            grad_soft = nt(da, vv[u])
            low, grads = [], []
            for h in range(2):
                p = prob[u, :, (2 * i + h) * 128 : (2 * i + h + 1) * 128]
                g = grad_soft[:, h * 128 : (h + 1) * 128]
                total = jnp.sum(p * g, axis=-1, keepdims=True)
                grads.append((p * (g - total) * SCALE).astype(BF16))
                low.append(p.astype(BF16))
            grads = jnp.concatenate(grads, axis=1)
            low = jnp.concatenate(low, axis=1)
            gq = nn(grads, kk[u])
            gpr[m, slot, i * 128 : (i + 1) * 128] = (gq * rope[0] - partner(gq) * rope[1]).astype(BF16)
            acc_k = acc_k + tn(grads, q_rot[u, :, i * 128 : (i + 1) * 128])
            acc_v = acc_v + tn(low, da)
        grad_k = acc_k[0:128] + pltpu.roll(acc_k[128:256], HD, 1)
        grad_v = pltpu.roll(acc_v[0:128], HD, 1) + acc_v[128:256]
        both = jnp.where(first_head, grad_k, grad_v)
        gpr[m, slot, 512:640] = (both * rope[2] - partner(both) * rope[3]).astype(BF16)
        gp = gpr[m, slot, :]
        for i in range(width // 512):
            gn[u, :, i * 512 : (i + 1) * 512] = nt(gp, wq[m, i * 512 : (i + 1) * 512, :]).astype(BF16)

    scatters = {}

    def scatter(u):
        scatters[u] = [
            send(
                gn.at[u, pl.ds(pl.multiple_of(tensor_peer(k) * rows, rows), rows)],
                rsr.at[u, k - 1],
                rs_s.at[u, k - 1],
                rs_r.at[u, k - 1],
                (s, tensor_peer(k), j),
            )
            for k in (1, 3, 2)
        ]

    def finish(u):
        t, m = u // 2, u % 2
        for copy in scatters[u]:
            copy.wait_recv()
        total = gn[u, own, :].astype(F32)
        for k in range(3):
            total = total + rsr[u, k].astype(F32)
        x = xg[u, own, :].astype(F32)
        inverse = lax.rsqrt(jnp.mean(x * x, axis=-1, keepdims=True) + EPSILON)
        unit = x * inverse
        g = total * gain[m : m + 1, :]
        result = dyg[u, own, :].astype(F32) + inverse * (g - unit * jnp.mean(g * unit, axis=-1, keepdims=True))
        ug[u] = result.astype(BF16)
        scale = jnp.sum(total * unit, axis=0, keepdims=True)
        if t == 0:
            gain_sum[m : m + 1, :] = scale
        else:
            gain_sum[m : m + 1, :] = gain_sum[m : m + 1, :] + scale

    def shift_copy(m):
        step = 1 if m == 1 else -1
        return pltpu.make_async_remote_copy(
            src_ref=ug.at[m],
            dst_ref=dyg.at[2 + m, own],
            send_sem=sh_s.at[m],
            recv_sem=sh_r.at[m],
            device_id=(lax.rem(s + step + n_s, n_s), c, j),
            device_id_type=MESH,
        )

    def sends(m):
        return s < n_s - 1 if m == 1 else s > 0

    def receives(m):
        return s > 0 if m == 1 else s < n_s - 1

    top_copy = pltpu.make_async_copy(t_hbm, dyg.at[3, own], own_sem.at[6])
    turn_copy = pltpu.make_async_copy(ug.at[1], dyg.at[2, own], own_sem.at[7])

    def shift(m):
        pl.when(sends(m))(lambda: shift_copy(m).start())
        if m == 1:
            pl.when(s == 0)(lambda: top_copy.start())
            pl.when(s == n_s - 1)(lambda: turn_copy.start())

    def shifted(m):
        pl.when(receives(m))(lambda: shift_copy(m).wait_recv())
        pl.when(jnp.logical_not(receives(m)))(lambda: (top_copy if m == 1 else turn_copy).wait())

    dp_order = (1, 4, 3, 5, 7, 2, 6)
    normed_copies, grad_copies, part_copies = {}, {}, {}
    own_normed = {}

    def spread_normed(u):
        t, m = u // 2, u % 2
        lanes = pl.ds(pl.multiple_of((j * 2 + t) * 128, 128), 128)
        own_normed[u] = pltpu.make_async_copy(
            n_t.at[u, pl.ds(pl.multiple_of(j * slice_q, slice_q), slice_q)], n_tr.at[m, :, lanes], own_sem.at[8 + u]
        )
        own_normed[u].start()
        normed_copies[u] = [
            send(
                n_t.at[u, pl.ds(pl.multiple_of(dp_peer(k) * slice_q, slice_q), slice_q)],
                n_tr.at[m, :, lanes],
                nt_s.at[u, k - 1],
                nt_r.at[u, k - 1],
                (s, c, dp_peer(k)),
            )
            for k in dp_order
        ]

    def spread_grad(u):
        t, m = u // 2, u % 2
        slot = pl.ds(pl.multiple_of((j * 2 + t) * 128, 128), 128)
        grad_copies[u] = [
            send(gpr.at[m, slot], gpr.at[m, slot], gp_s.at[u, k - 1], gp_r.at[u, k - 1], (s, c, dp_peer(k)))
            for k in dp_order
        ]

    def out_part(m):
        both_t = jnp.concatenate([dyg[m], dyg[2 + m]], axis=0)
        for i in range(width // 512):
            part[m, :, i * 512 : (i + 1) * 512] = tn(att[m], both_t[:, i * 512 : (i + 1) * 512]).astype(BF16)

    def spread_out(m):
        part_copies[m] = [
            send(
                part.at[m, pl.ds(pl.multiple_of(dp_peer(k) * slice_o, slice_o), slice_o)],
                part_r.at[m, k - 1],
                po_s.at[m, k - 1],
                po_r.at[m, k - 1],
                (s, c, dp_peer(k)),
            )
            for k in dp_order
        ]

    gather_x(1)
    gather_d(1)
    gather_x(0)
    gather_d(0)

    loads["gain"].wait()
    loads["rope"].wait()
    gathered("x", 1)
    loads["wq1"].wait()
    forward(1)
    spread_normed(1)
    gathered("d", 1)
    loads["wo1"].wait()
    backward(1)
    scatter(1)
    gather_x(3)
    gathered("x", 0)
    loads["wq0"].wait()
    forward(0)
    gathered("d", 0)
    loads["wo0"].wait()
    backward(0)
    scatter(0)
    gather_x(2)
    finish(1)
    shift(1)
    finish(0)
    shift(0)
    spread_normed(0)
    spread_grad(1)
    spread_grad(0)
    gathered("x", 3)
    forward(3)
    shifted(1)
    gather_d(3)
    gathered("x", 2)
    shifted(0)
    gather_d(2)
    forward(2)
    spread_normed(3)
    spread_normed(2)
    gathered("d", 3)
    out_part(1)
    spread_out(1)
    backward(3)
    scatter(3)
    spread_grad(3)
    gathered("d", 2)
    out_part(0)
    spread_out(0)
    backward(2)
    scatter(2)
    spread_grad(2)
    finish(3)
    finish(2)
    ug_copy = pltpu.make_async_copy(ug, ug_out, out_sem.at[0])
    ug_copy.start()

    g1[c] = gain_sum[...]
    first = [
        send(g1.at[c], g1.at[c], g1_s.at[k - 1], g1_r.at[k - 1], (s, tensor_peer(k), j)) for k in (1, 2, 3)
    ]
    for copy in first:
        copy.wait_recv()
    g2[j] = ((g1[0] + g1[1]) + g1[2]) + g1[3]
    second = [send(g2.at[j], g2.at[j], g2_s.at[k - 1], g2_r.at[k - 1], (s, c, dp_peer(k))) for k in range(1, 8)]

    outs = []
    for m in (1, 0):
        for u in (m, 2 + m):
            own_normed[u].wait()
            for copy in normed_copies[u]:
                copy.wait_recv()
            for copy in grad_copies[u]:
                copy.wait_recv()
        gq_v[m] = nn(n_tr[m], gpr[m]).astype(BF16)
        outs.append(pltpu.make_async_copy(gq_v.at[m], gq_out.at[m], out_sem.at[1 + m]))
        outs[-1].start()
    for m in (1, 0):
        for copy in part_copies[m]:
            copy.wait_recv()
        total = part[m, pl.ds(pl.multiple_of(j * slice_o, slice_o), slice_o), :].astype(F32)
        for k in range(n_j - 1):
            total = total + part_r[m, k].astype(F32)
        go_v[m] = total.astype(BF16)
        outs.append(pltpu.make_async_copy(go_v.at[m], go_out.at[m], out_sem.at[3 + m]))
        outs[-1].start()
    for copy in second:
        copy.wait_recv()
    total = g2[0]
    for k in range(1, n_j):
        total = total + g2[k]
    gg_v[...] = total
    outs.append(pltpu.make_async_copy(gg_v, gg_out, out_sem.at[5]))
    outs[-1].start()

    for m in (0, 1):
        pl.when(sends(m))(lambda m=m: shift_copy(m).wait_send())
    for copy in sent:
        copy.wait_send()
    ug_copy.wait()
    for copy in outs:
        copy.wait()


def local(layer_in, carry_in, top_grad, w_qkv, w_out, gain):
    ticks, members = layer_in.shape[:2]
    rows, width = layer_in.shape[-2:]
    n_c, n_j = DIMS["tensor"], DIMS["dp"]
    length = rows * n_c
    units = ticks * members
    x = layer_in.reshape(units, rows, width)
    carry = carry_in.reshape(members, rows, width)
    top = top_grad.reshape(rows, width)
    wq = w_qkv[:, 0]
    wo = w_out[:, 0]
    cols, heads = wq.shape[2], wo.shape[1]
    slice_q, slice_o = width // n_j, heads // n_j
    tokens = n_j * ticks * length
    hbm = pl.BlockSpec(memory_space=pl.ANY)
    dma = pltpu.SemaphoreType.DMA
    outs = pl.pallas_call(
        kernel,
        out_shape=(
            jax.ShapeDtypeStruct((units, rows, width), BF16),
            jax.ShapeDtypeStruct((members, slice_q, cols), BF16),
            jax.ShapeDtypeStruct((members, slice_o, width), BF16),
            jax.ShapeDtypeStruct((members, width), F32),
        ),
        in_specs=[hbm] * 7,
        out_specs=(hbm,) * 4,
        scratch_shapes=[
            pltpu.VMEM((members, width, cols), BF16),
            pltpu.VMEM((members, heads, width), BF16),
            pltpu.VMEM((members, width), F32),
            pltpu.VMEM((4, length, 128), F32),
            pltpu.VMEM((units, length, width), BF16),
            pltpu.VMEM((units, length, width), BF16),
            pltpu.VMEM((units, width, length), BF16),
            pltpu.VMEM((members, slice_q, tokens), BF16),
            pltpu.VMEM((members, tokens, cols), BF16),
            pltpu.VMEM((units, length, heads), BF16),
            pltpu.VMEM((units, 256, 128), BF16),
            pltpu.VMEM((units, 256, 128), BF16),
            pltpu.VMEM((units, length, GROUP * 128), F32),
            pltpu.VMEM((members, ticks * length, heads), BF16),
            pltpu.VMEM((units, length, width), BF16),
            pltpu.VMEM((units, 3, rows, width), BF16),
            pltpu.VMEM((units, rows, width), BF16),
            pltpu.VMEM((members, heads, width), BF16),
            pltpu.VMEM((members, n_j - 1, slice_o, width), BF16),
            pltpu.VMEM((members, width), F32),
            pltpu.VMEM((n_c, members, width), F32),
            pltpu.VMEM((n_j, members, width), F32),
            pltpu.VMEM((members, slice_q, cols), BF16),
            pltpu.VMEM((members, slice_o, width), BF16),
            pltpu.VMEM((members, width), F32),
            dma((6,)), dma((12,)), dma((6,)),
            dma((4, 3)), dma((4, 3)), dma((4, 3)), dma((4, 3)), dma((4, 3)), dma((4, 3)), dma((2,)), dma((2,)),
            dma((4, 7)), dma((4, 7)), dma((4, 7)), dma((4, 7)), dma((2, 7)), dma((2, 7)),
            dma((3,)), dma((3,)), dma((7,)), dma((7,)),
        ],
        compiler_params=pltpu.CompilerParams(has_side_effects=True, vmem_limit_bytes=63 * 1024 * 1024),
    )(x, carry, top, wq, wo, gain[:, 0], rope_tables(length))
    unit_grads, grad_qkv, grad_out, grad_gain = outs
    return (
        unit_grads.reshape(ticks, members, 1, 1, rows, width),
        grad_qkv[:, None],
        grad_out[:, None],
        grad_gain[:, None],
    )


def solution(mesh):
    in_specs = (
        P(None, None, "section", "dp", "tensor", None),
        P(None, "section", "dp", "tensor", None),
        P(None, "dp", "tensor", None),
        P(None, "section", None, "tensor"),
        P(None, "section", "tensor", None),
        P(None, "section", None),
    )
    out_specs = (
        P(None, None, "section", "dp", "tensor", None),
        P(None, "section", "dp", "tensor"),
        P(None, "section", ("tensor", "dp"), None),
        P(None, "section", None),
    )
    return jax.shard_map(local, mesh=mesh, in_specs=in_specs, out_specs=out_specs, check_vma=False)
```

```python
import functools
import math

import jax
import jax.numpy as jnp
from jax import lax
from jax.experimental import pallas as pl
from jax.experimental.pallas import tpu as pltpu
from jax.sharding import PartitionSpec as P

HD = 64
GROUP = 8
EPSILON = 1e-06
ROPE_BASE = 1000000.0
SCALE = 1.0 / math.sqrt(HD)
F32 = jnp.float32
BF16 = jnp.bfloat16
MESH = pl.DeviceIdType.MESH
DIMS = dict(ticks=2, sections=4, tensor=4, dp=8)


def rope_tables(length):
    half = HD // 2
    exponent = jnp.arange(half, dtype=F32) * (2.0 / HD)
    frequency = ROPE_BASE ** (-exponent)
    angle = jnp.arange(length, dtype=F32)[:, None] * frequency[None, :]
    cosine, sine = jnp.cos(angle), jnp.sin(angle)
    head_cos = jnp.concatenate([cosine, cosine], axis=1)
    head_sin = jnp.concatenate([-sine, sine], axis=1)
    return jnp.stack(
        [
            jnp.concatenate([head_cos, head_cos], axis=1),
            jnp.concatenate([head_sin, head_sin], axis=1),
            jnp.concatenate([head_cos, jnp.ones_like(head_cos)], axis=1),
            jnp.concatenate([head_sin, jnp.zeros_like(head_sin)], axis=1),
        ]
    )


def nt(a, b):
    return lax.dot_general(a, b, (((1,), (1,)), ((), ())), preferred_element_type=F32)


def tn(a, b):
    return lax.dot_general(a, b, (((0,), (0,)), ((), ())), preferred_element_type=F32)


def nn(a, b):
    return jnp.dot(a, b, preferred_element_type=F32)


def kernel(
    x_hbm, c_hbm, t_hbm, wq_hbm, wo_hbm, gain_hbm, rope_hbm,
    ug_out, gq_out, go_out, gg_out,
    wq, wo, gain, rope, xg, dyg, n_t, n_tr, gpr, q_rot, kk, vv, prob, att, gn, rsr, ug,
    dy_far, att_far, part, part_r, wq_part, wq_part_r, gain_sum, g1, g2, g3, gq_v, gq_low, go_v, go_far, gg_v,
    w_sem, own_sem, out_sem, ag_s, ag_r, dy_s, dy_r, rs_s, rs_r, sh_s, sh_r,
    nt_s, nt_r, gp_s, gp_r, pair_s, pair_r, po_s, po_r, g1_s, g1_r, g2_s, g2_r,
):
    s, c, j = lax.axis_index("section"), lax.axis_index("tensor"), lax.axis_index("dp")
    n_s, n_c, n_j = DIMS["sections"], DIMS["tensor"], DIMS["dp"]
    rows = x_hbm.shape[1]
    length = rows * n_c
    width = x_hbm.shape[2]
    slice_q = gq_out.shape[1]
    slice_o = go_out.shape[1]
    own = pl.ds(pl.multiple_of(c * rows, rows), rows)
    lane = lax.broadcasted_iota(jnp.int32, (length, 128), 1)
    low_half = (lane % HD) < (HD // 2)
    first_head = lane < HD

    def tensor_peer(k):
        return lax.rem(c + k, n_c)

    z, y = lax.rem(j, 4), lax.div(j, 4)
    far = (1 - y) * 4 + z
    half = width // 2
    half_lanes = pl.ds(pl.multiple_of(y * half, half), half)
    far_lanes = pl.ds(pl.multiple_of((1 - y) * half, half), half)

    def z_peer(k):
        return lax.rem(z + k, 4)

    def at_z(k):
        return (s, c, y * 4 + z_peer(k))

    pair = (s, c, far)
    z_order = (1, 3, 2)

    sent = []

    def send(src, dst, s_sem, r_sem, to):
        copy = pltpu.make_async_remote_copy(
            src_ref=src, dst_ref=dst, send_sem=s_sem, recv_sem=r_sem, device_id=to, device_id_type=MESH
        )
        copy.start()
        sent.append(copy)
        return copy

    loads = {}

    def load(name, src, dst, i):
        loads[name] = pltpu.make_async_copy(src, dst, w_sem.at[i])
        loads[name].start()

    load("gain", gain_hbm, gain, 0)
    load("rope", rope_hbm, rope, 1)
    own_copies = {}
    for i, (name, src, dst) in enumerate(
        [(("x", u), x_hbm.at[u], xg.at[u, own]) for u in range(4)]
        + [(("d", u), c_hbm.at[u], dyg.at[u, own]) for u in range(2)]
    ):
        own_copies[name] = pltpu.make_async_copy(src, dst, own_sem.at[i])
        own_copies[name].start()
    barrier = pltpu.get_barrier_semaphore()
    friends = [(s, tensor_peer(k), j) for k in (1, 2, 3)] + [at_z(k) for k in (1, 2, 3)]
    friends += [pair, (lax.rem(s + 1, n_s), c, j), (lax.rem(s + n_s - 1, n_s), c, j)]
    for friend in friends:
        pl.semaphore_signal(barrier, inc=1, device_id=friend, device_id_type=MESH)
    load("wq1", wq_hbm.at[1], wq.at[1], 2)
    load("wo1", wo_hbm.at[1], wo.at[1], 3)
    load("wq0", wq_hbm.at[0], wq.at[0], 4)
    load("wo0", wo_hbm.at[0], wo.at[0], 5)

    pl.semaphore_wait(barrier, len(friends))

    gathers = {}

    def gather_x(u):
        gathers["x", u] = [
            send(x_hbm.at[u], xg.at[u, own], ag_s.at[u, k - 1], ag_r.at[u, k - 1], (s, tensor_peer(k), j))
            for k in (1, 3, 2)
        ]

    def gather_d(u):
        src = c_hbm.at[u] if u < 2 else dyg.at[u, own]
        gathers["d", u] = [
            send(src, dyg.at[u, own], dy_s.at[u, k - 1], dy_r.at[u, k - 1], (s, tensor_peer(k), j))
            for k in (1, 3, 2)
        ]

    def gathered(kind, u):
        if (kind, u) in own_copies:
            own_copies[kind, u].wait()
        for copy in gathers[kind, u]:
            copy.wait_recv()

    def partner(chunk):
        return jnp.where(low_half, pltpu.roll(chunk, 96, 1), pltpu.roll(chunk, 32, 1))

    def forward(u):
        t, m = u // 2, u % 2
        x = xg[u].astype(F32)
        inverse = lax.rsqrt(jnp.mean(x * x, axis=-1, keepdims=True) + EPSILON)
        normed = (x * inverse * gain[m : m + 1, :]).astype(BF16)
        for i in range(width // 256):
            n_t[u, i * 256 : (i + 1) * 256, :] = jnp.transpose(normed[:, i * 256 : (i + 1) * 256])
        projected = nn(normed, wq[m])
        for i in range(4):
            chunk = projected[:, i * 128 : (i + 1) * 128]
            q_rot[u, :, i * 128 : (i + 1) * 128] = (chunk * rope[0] + partner(chunk) * rope[1]).astype(BF16)
        chunk = projected[:, 512:640]
        both = (chunk * rope[2] + partner(chunk) * rope[3]).astype(BF16).astype(F32)
        key_low = jnp.where(first_head, both, 0.0)
        value_high = jnp.where(first_head, 0.0, both)
        kk[u, 0:128, :] = key_low.astype(BF16)
        kk[u, 128:256, :] = pltpu.roll(key_low, HD, 1).astype(BF16)
        vv[u, 0:128, :] = pltpu.roll(value_high, HD, 1).astype(BF16)
        vv[u, 128:256, :] = value_high.astype(BF16)
        causal = lax.broadcasted_iota(jnp.int32, (length, length), 0) >= lax.broadcasted_iota(
            jnp.int32, (length, length), 1
        )
        for i in range(4):
            scores = nt(q_rot[u, :, i * 128 : (i + 1) * 128], kk[u]) * SCALE
            low = []
            for h in range(2):
                part_scores = jnp.where(causal, scores[:, h * 128 : (h + 1) * 128], -1e30)
                e = jnp.exp(part_scores - jnp.max(part_scores, axis=-1, keepdims=True))
                p = e / jnp.sum(e, axis=-1, keepdims=True)
                prob[u, :, (2 * i + h) * 128 : (2 * i + h + 1) * 128] = p
                low.append(p.astype(BF16))
            att[m, t * 128 : (t + 1) * 128, i * 128 : (i + 1) * 128] = nn(
                jnp.concatenate(low, axis=1), vv[u]
            ).astype(BF16)

    def backward(u):
        t, m = u // 2, u % 2
        grad_att = nt(dyg[u], wo[m]).astype(BF16)
        acc_k = jnp.zeros((256, 128), F32)
        acc_v = jnp.zeros((256, 128), F32)
        slot = pl.ds(pl.multiple_of((z * 2 + t) * 128, 128), 128)
        for i in range(4):
            da = grad_att[:, i * 128 : (i + 1) * 128]
            grad_soft = nt(da, vv[u])
            low, grads = [], []
            for h in range(2):
                p = prob[u, :, (2 * i + h) * 128 : (2 * i + h + 1) * 128]
                g = grad_soft[:, h * 128 : (h + 1) * 128]
                total = jnp.sum(p * g, axis=-1, keepdims=True)
                grads.append((p * (g - total) * SCALE).astype(BF16))
                low.append(p.astype(BF16))
            grads = jnp.concatenate(grads, axis=1)
            low = jnp.concatenate(low, axis=1)
            gq = nn(grads, kk[u])
            gpr[m, slot, i * 128 : (i + 1) * 128] = (gq * rope[0] - partner(gq) * rope[1]).astype(BF16)
            acc_k = acc_k + tn(grads, q_rot[u, :, i * 128 : (i + 1) * 128])
            acc_v = acc_v + tn(low, da)
        grad_k = acc_k[0:128] + pltpu.roll(acc_k[128:256], HD, 1)
        grad_v = pltpu.roll(acc_v[0:128], HD, 1) + acc_v[128:256]
        both = jnp.where(first_head, grad_k, grad_v)
        gpr[m, slot, 512:640] = (both * rope[2] - partner(both) * rope[3]).astype(BF16)
        gp = gpr[m, slot, :]
        for i in range(width // 512):
            gn[u, :, i * 512 : (i + 1) * 512] = nt(gp, wq[m, i * 512 : (i + 1) * 512, :]).astype(BF16)

    scatters = {}

    def scatter(u):
        scatters[u] = [
            send(
                gn.at[u, pl.ds(pl.multiple_of(tensor_peer(k) * rows, rows), rows)],
                rsr.at[u, k - 1],
                rs_s.at[u, k - 1],
                rs_r.at[u, k - 1],
                (s, tensor_peer(k), j),
            )
            for k in (1, 3, 2)
        ]

    def finish(u):
        t, m = u // 2, u % 2
        for copy in scatters[u]:
            copy.wait_recv()
        total = gn[u, own, :].astype(F32)
        for k in range(3):
            total = total + rsr[u, k].astype(F32)
        x = xg[u, own, :].astype(F32)
        inverse = lax.rsqrt(jnp.mean(x * x, axis=-1, keepdims=True) + EPSILON)
        unit = x * inverse
        g = total * gain[m : m + 1, :]
        result = dyg[u, own, :].astype(F32) + inverse * (g - unit * jnp.mean(g * unit, axis=-1, keepdims=True))
        ug[u] = result.astype(BF16)
        scale = jnp.sum(total * unit, axis=0, keepdims=True)
        if t == 0:
            gain_sum[m : m + 1, :] = scale
        else:
            gain_sum[m : m + 1, :] = gain_sum[m : m + 1, :] + scale

    def shift_copy(m):
        step = 1 if m == 1 else -1
        return pltpu.make_async_remote_copy(
            src_ref=ug.at[m],
            dst_ref=dyg.at[2 + m, own],
            send_sem=sh_s.at[m],
            recv_sem=sh_r.at[m],
            device_id=(lax.rem(s + step + n_s, n_s), c, j),
            device_id_type=MESH,
        )

    def sends(m):
        return s < n_s - 1 if m == 1 else s > 0

    def receives(m):
        return s > 0 if m == 1 else s < n_s - 1

    top_copy = pltpu.make_async_copy(t_hbm, dyg.at[3, own], own_sem.at[6])
    turn_copy = pltpu.make_async_copy(ug.at[1], dyg.at[2, own], own_sem.at[7])

    def shift(m):
        pl.when(sends(m))(lambda: shift_copy(m).start())
        if m == 1:
            pl.when(s == 0)(lambda: top_copy.start())
            pl.when(s == n_s - 1)(lambda: turn_copy.start())

    def shifted(m):
        pl.when(receives(m))(lambda: shift_copy(m).wait_recv())
        pl.when(jnp.logical_not(receives(m)))(lambda: (top_copy if m == 1 else turn_copy).wait())

    normed_copies, grad_copies, part_copies, pair_copies = {}, {}, {}, {}
    own_normed = {}

    def rows_of(block, size):
        return pl.ds(pl.multiple_of(block * size, size), size)

    def spread_normed(u):
        t, m = u // 2, u % 2
        lanes = pl.ds(pl.multiple_of((z * 2 + t) * 128, 128), 128)
        own_normed[u] = []
        normed_copies[u] = []
        for b in range(2):
            copy = pltpu.make_async_copy(
                n_t.at[u, rows_of(b * 4 + z, slice_q)], n_tr.at[m, b, :, lanes], own_sem.at[8 + u * 2 + b]
            )
            copy.start()
            own_normed[u].append(copy)
        for k in z_order:
            for b in range(2):
                normed_copies[u].append(
                    send(
                        n_t.at[u, rows_of(b * 4 + z_peer(k), slice_q)],
                        n_tr.at[m, b, :, lanes],
                        nt_s.at[u, b, k - 1],
                        nt_r.at[u, b, k - 1],
                        at_z(k),
                    )
                )

    def spread_grad(u):
        t, m = u // 2, u % 2
        slot = pl.ds(pl.multiple_of((z * 2 + t) * 128, 128), 128)
        grad_copies[u] = [
            send(gpr.at[m, slot], gpr.at[m, slot], gp_s.at[u, k - 1], gp_r.at[u, k - 1], at_z(k))
            for k in z_order
        ]

    def pair_send(name, i, src, dst):
        pair_copies[name] = send(src, dst, pair_s.at[i], pair_r.at[i], pair)

    def share_attended(u):
        t, m = u // 2, u % 2
        mine = att.at[m, t * 128 : (t + 1) * 128]
        pair_send(("att", u), u, mine, att_far.at[m, t * 128 : (t + 1) * 128])

    def share_dy(u):
        pair_send(("dy", u), 4 + u, dyg.at[u, :, far_lanes], dy_far.at[u])

    def out_part(m):
        for u in (m, 2 + m):
            pair_copies["att", u].wait_recv()
            pair_copies["dy", u].wait_recv()
        lhs = jnp.concatenate([att[m], att_far[m]], axis=0)
        rhs = jnp.concatenate([dyg[m, :, half_lanes], dyg[2 + m, :, half_lanes], dy_far[m], dy_far[2 + m]], axis=0)
        for i in range(half // 256):
            part[m, :, i * 256 : (i + 1) * 256] = tn(lhs, rhs[:, i * 256 : (i + 1) * 256]).astype(BF16)

    def spread_out(m):
        part_copies[m] = []
        for k in z_order:
            for b in range(2):
                part_copies[m].append(
                    send(
                        part.at[m, rows_of(b * 4 + z_peer(k), slice_o)],
                        part_r.at[m, b, k - 1],
                        po_s.at[m, b, k - 1],
                        po_r.at[m, b, k - 1],
                        at_z(k),
                    )
                )

    def out_sum(m):
        for copy in part_copies[m]:
            copy.wait_recv()
        for b in (1 - y, y):
            total = part[m, rows_of(b * 4 + z, slice_o), :].astype(F32)
            for k in range(3):
                total = total + part_r[m, b, k].astype(F32)
            if b is y:
                go_v[m, :, half_lanes] = total.astype(BF16)
            else:
                go_far[m] = total.astype(BF16)
                pair_send(("out", m), 8 + m, go_far.at[m], go_v.at[m, :, half_lanes])

    def qkv_part(m):
        for u in (m, 2 + m):
            for copy in own_normed[u]:
                copy.wait()
            for copy in normed_copies[u] + grad_copies[u]:
                copy.wait_recv()
        wq_part[m] = nn(n_tr[m, 1 - y], gpr[m]).astype(BF16)
        pair_send(("wq", m), 10 + m, wq_part.at[m], wq_part_r.at[m])
        return nn(n_tr[m, y], gpr[m])

    gather_x(1)
    gather_d(1)
    gather_x(0)
    gather_d(0)

    loads["gain"].wait()
    loads["rope"].wait()
    gathered("x", 1)
    loads["wq1"].wait()
    forward(1)
    spread_normed(1)
    share_attended(1)
    gathered("d", 1)
    share_dy(1)
    loads["wo1"].wait()
    backward(1)
    scatter(1)
    gather_x(3)
    spread_grad(1)
    gathered("x", 0)
    loads["wq0"].wait()
    forward(0)
    spread_normed(0)
    share_attended(0)
    gathered("d", 0)
    share_dy(0)
    loads["wo0"].wait()
    backward(0)
    scatter(0)
    gather_x(2)
    spread_grad(0)
    finish(1)
    shift(1)
    finish(0)
    shift(0)
    gathered("x", 3)
    forward(3)
    share_attended(3)
    shifted(1)
    gather_d(3)
    gathered("x", 2)
    shifted(0)
    gather_d(2)
    spread_normed(3)
    forward(2)
    share_attended(2)
    spread_normed(2)
    gathered("d", 3)
    share_dy(3)
    backward(3)
    scatter(3)
    spread_grad(3)
    out_part(1)
    spread_out(1)
    gathered("d", 2)
    share_dy(2)
    backward(2)
    scatter(2)
    spread_grad(2)
    out_part(0)
    spread_out(0)
    outs = []

    def put(src, dst, i):
        outs.append(pltpu.make_async_copy(src, dst, out_sem.at[i]))
        outs[-1].start()

    gq_v[1] = qkv_part(1)
    finish(3)
    out_sum(1)
    finish(2)
    put(ug, ug_out, 0)

    g1[c] = gain_sum[...]
    first = [send(g1.at[c], g1.at[c], g1_s.at[k - 1], g1_r.at[k - 1], (s, tensor_peer(k), j)) for k in (1, 2, 3)]
    gq_v[0] = qkv_part(0)
    for copy in first:
        copy.wait_recv()
    g2[z] = ((g1[0] + g1[1]) + g1[2]) + g1[3]
    second = [send(g2.at[z], g2.at[z], g2_s.at[k - 1], g2_r.at[k - 1], at_z(k)) for k in (1, 2, 3)]
    out_sum(0)
    for copy in second:
        copy.wait_recv()
    g3[y] = ((g2[0] + g2[1]) + g2[2]) + g2[3]
    pair_send("gain", 12, g3.at[y], g3.at[y])
    for m in (1, 0):
        pair_copies["wq", m].wait_recv()
        gq_low[m] = (gq_v[m] + wq_part_r[m].astype(F32)).astype(BF16)
        put(gq_low.at[m], gq_out.at[m], 1 + m)
    for m in (1, 0):
        pair_copies["out", m].wait_recv()
        put(go_v.at[m], go_out.at[m], 3 + m)
    pair_copies["gain"].wait_recv()
    gg_v[...] = g3[0] + g3[1]
    put(gg_v, gg_out, 5)

    for m in (0, 1):
        pl.when(sends(m))(lambda m=m: shift_copy(m).wait_send())
    for copy in sent:
        copy.wait_send()
    for copy in outs:
        copy.wait()


def local(layer_in, carry_in, top_grad, w_qkv, w_out, gain):
    ticks, members = layer_in.shape[:2]
    rows, width = layer_in.shape[-2:]
    n_c, n_j = DIMS["tensor"], DIMS["dp"]
    length = rows * n_c
    units = ticks * members
    x = layer_in.reshape(units, rows, width)
    carry = carry_in.reshape(members, rows, width)
    top = top_grad.reshape(rows, width)
    wq = w_qkv[:, 0]
    wo = w_out[:, 0]
    cols, heads = wq.shape[2], wo.shape[1]
    slice_q, slice_o = width // n_j, heads // n_j
    tokens = 4 * ticks * length
    hbm = pl.BlockSpec(memory_space=pl.ANY)
    dma = pltpu.SemaphoreType.DMA
    outs = pl.pallas_call(
        kernel,
        out_shape=(
            jax.ShapeDtypeStruct((units, rows, width), BF16),
            jax.ShapeDtypeStruct((members, slice_q, cols), BF16),
            jax.ShapeDtypeStruct((members, slice_o, width), BF16),
            jax.ShapeDtypeStruct((members, width), F32),
        ),
        in_specs=[hbm] * 7,
        out_specs=(hbm,) * 4,
        scratch_shapes=[
            pltpu.VMEM((members, width, cols), BF16),
            pltpu.VMEM((members, heads, width), BF16),
            pltpu.VMEM((members, width), F32),
            pltpu.VMEM((4, length, 128), F32),
            pltpu.VMEM((units, length, width), BF16),
            pltpu.VMEM((units, length, width), BF16),
            pltpu.VMEM((units, width, length), BF16),
            pltpu.VMEM((members, 2, slice_q, tokens), BF16),
            pltpu.VMEM((members, tokens, cols), BF16),
            pltpu.VMEM((units, length, heads), BF16),
            pltpu.VMEM((units, 256, 128), BF16),
            pltpu.VMEM((units, 256, 128), BF16),
            pltpu.VMEM((units, length, GROUP * 128), F32),
            pltpu.VMEM((members, ticks * length, heads), BF16),
            pltpu.VMEM((units, length, width), BF16),
            pltpu.VMEM((units, 3, rows, width), BF16),
            pltpu.VMEM((units, rows, width), BF16),
            pltpu.VMEM((units, length, width // 2), BF16),
            pltpu.VMEM((members, ticks * length, heads), BF16),
            pltpu.VMEM((members, heads, width // 2), BF16),
            pltpu.VMEM((members, 2, 3, slice_o, width // 2), BF16),
            pltpu.VMEM((members, slice_q, cols), BF16),
            pltpu.VMEM((members, slice_q, cols), BF16),
            pltpu.VMEM((members, width), F32),
            pltpu.VMEM((n_c, members, width), F32),
            pltpu.VMEM((4, members, width), F32),
            pltpu.VMEM((2, members, width), F32),
            pltpu.VMEM((members, slice_q, cols), F32),
            pltpu.VMEM((members, slice_q, cols), BF16),
            pltpu.VMEM((members, slice_o, width), BF16),
            pltpu.VMEM((members, slice_o, width // 2), BF16),
            pltpu.VMEM((members, width), F32),
            dma((6,)), dma((16,)), dma((6,)),
            dma((4, 3)), dma((4, 3)), dma((4, 3)), dma((4, 3)), dma((4, 3)), dma((4, 3)), dma((2,)), dma((2,)),
            dma((4, 2, 3)), dma((4, 2, 3)), dma((4, 3)), dma((4, 3)), dma((13,)), dma((13,)),
            dma((2, 2, 3)), dma((2, 2, 3)), dma((3,)), dma((3,)), dma((3,)), dma((3,)),
        ],
        compiler_params=pltpu.CompilerParams(has_side_effects=True, collective_id=0, vmem_limit_bytes=63 * 1024 * 1024),
    )(x, carry, top, wq, wo, gain[:, 0], rope_tables(length))
    unit_grads, grad_qkv, grad_out, grad_gain = outs
    return (
        unit_grads.reshape(ticks, members, 1, 1, rows, width),
        grad_qkv[:, None],
        grad_out[:, None],
        grad_gain[:, None],
    )


def solution(mesh):
    in_specs = (
        P(None, None, "section", "dp", "tensor", None),
        P(None, "section", "dp", "tensor", None),
        P(None, "dp", "tensor", None),
        P(None, "section", None, "tensor"),
        P(None, "section", "tensor", None),
        P(None, "section", None),
    )
    out_specs = (
        P(None, None, "section", "dp", "tensor", None),
        P(None, "section", "dp", "tensor"),
        P(None, "section", ("tensor", "dp"), None),
        P(None, "section", None),
    )
    return jax.shard_map(local, mesh=mesh, in_specs=in_specs, out_specs=out_specs, check_vma=False)
```

```python
import functools
import math

import jax
import jax.numpy as jnp
import numpy as np
from jax import lax
from jax.experimental import pallas as pl
from jax.experimental.pallas import tpu as pltpu
from jax.sharding import PartitionSpec as P

HD = 64
GROUP = 8
EPSILON = 1e-06
ROPE_BASE = 1000000.0
SCALE = 1.0 / math.sqrt(HD)
F32 = jnp.float32
BF16 = jnp.bfloat16
MESH = pl.DeviceIdType.MESH
DIMS = dict(ticks=2, sections=4, tensor=4, dp=8)


def rope_tables(length):
    half = HD // 2
    exponent = np.arange(half, dtype=np.float32) * np.float32(2.0 / HD)
    frequency = np.power(np.float32(ROPE_BASE), -exponent).astype(np.float32)
    angle = np.arange(length, dtype=np.float32)[:, None] * frequency[None, :]
    cosine, sine = np.cos(angle), np.sin(angle)
    head_cos = np.concatenate([cosine, cosine], axis=1)
    head_sin = np.concatenate([-sine, sine], axis=1)
    return np.stack(
        [
            np.concatenate([head_cos, head_cos], axis=1),
            np.concatenate([head_sin, head_sin], axis=1),
            np.concatenate([head_cos, np.ones_like(head_cos)], axis=1),
            np.concatenate([head_sin, np.zeros_like(head_sin)], axis=1),
        ]
    ).astype(np.float32)


def nt(a, b):
    return lax.dot_general(a, b, (((1,), (1,)), ((), ())), preferred_element_type=F32)


def tn(a, b):
    return lax.dot_general(a, b, (((0,), (0,)), ((), ())), preferred_element_type=F32)


def nn(a, b):
    return jnp.dot(a, b, preferred_element_type=F32)


def kernel(
    x_hbm, c_hbm, t_hbm, wq_hbm, wo_hbm, gain_hbm, rope_hbm,
    ug_out, gq_out, go_out, gg_out,
    wq, wo, gain, rope, xg, dyg, n_t, n_tr, gpr, q_rot, kk, vv, prob, att, gn, rsr, way, ug,
    dy_far, att_far, part, part_r, wq_part, wq_part_r, gain_sum, g1, g2, g3, gq_v, gq_low, go_v, go_far, gg_v,
    w_sem, own_sem, out_sem, ag_s, ag_r, dy_s, dy_r, rs_s, rs_r, sh_s, sh_r,
    nt_s, nt_r, gp_s, gp_r, pair_s, pair_r, po_s, po_r, g1_s, g1_r, g2_s, g2_r,
):
    s, c, j = lax.axis_index("section"), lax.axis_index("tensor"), lax.axis_index("dp")
    n_s, n_c, n_j = DIMS["sections"], DIMS["tensor"], DIMS["dp"]
    rows = x_hbm.shape[1]
    length = rows * n_c
    width = x_hbm.shape[2]
    slice_q = gq_out.shape[1]
    slice_o = go_out.shape[1]
    own = pl.ds(pl.multiple_of(c * rows, rows), rows)
    lane = lax.broadcasted_iota(jnp.int32, (length, 128), 1)
    low_half = (lane % HD) < (HD // 2)
    first_head = lane < HD

    def tensor_peer(k):
        return lax.rem(c + k, n_c)

    z, y = lax.rem(j, 4), lax.div(j, 4)
    far = (1 - y) * 4 + z
    half = width // 2
    half_lanes = pl.ds(pl.multiple_of(y * half, half), half)
    far_lanes = pl.ds(pl.multiple_of((1 - y) * half, half), half)

    def z_peer(k):
        return lax.rem(z + k, 4)

    def at_z(k):
        return (s, c, y * 4 + z_peer(k))

    pair = (s, c, far)
    z_order = (1, 3, 2)

    sent = []

    def send(src, dst, s_sem, r_sem, to):
        copy = pltpu.make_async_remote_copy(
            src_ref=src, dst_ref=dst, send_sem=s_sem, recv_sem=r_sem, device_id=to, device_id_type=MESH
        )
        copy.start()
        sent.append(copy)
        return copy

    loads = {}

    def load(name, src, dst, i):
        loads[name] = pltpu.make_async_copy(src, dst, w_sem.at[i])
        loads[name].start()

    load("gain", gain_hbm, gain, 0)
    load("rope", rope_hbm, rope, 1)
    own_copies = {}
    for i, (name, src, dst) in enumerate(
        [(("x", u), x_hbm.at[u], xg.at[u, own]) for u in range(4)]
        + [(("d", u), c_hbm.at[u], dyg.at[u, own]) for u in range(2)]
    ):
        own_copies[name] = pltpu.make_async_copy(src, dst, own_sem.at[i])
        own_copies[name].start()
    barrier = pltpu.get_barrier_semaphore()
    friends = [(s, tensor_peer(k), j) for k in (1, 2, 3)] + [at_z(k) for k in (1, 2, 3)]
    friends += [pair, (lax.rem(s + 1, n_s), c, j), (lax.rem(s + n_s - 1, n_s), c, j)]
    for friend in friends:
        pl.semaphore_signal(barrier, inc=1, device_id=friend, device_id_type=MESH)
    load("wq1", wq_hbm.at[1], wq.at[1], 2)
    load("wo1", wo_hbm.at[1], wo.at[1], 3)
    load("wq0", wq_hbm.at[0], wq.at[0], 4)
    load("wo0", wo_hbm.at[0], wo.at[0], 5)

    pl.semaphore_wait(barrier, len(friends))

    half_rows = rows // 2
    right, left = (s, tensor_peer(1), j), (s, tensor_peer(3), j)
    gathers = {}

    def block_half(block, h):
        return pl.ds(pl.multiple_of(block * rows + h * half_rows, half_rows), half_rows)

    def gather(kind, u):
        x_like = kind == "x"
        buf = xg.at[u] if x_like else dyg.at[u]
        src = x_hbm.at[u] if x_like else c_hbm.at[u] if u < 2 else dyg.at[u, own]
        ss, rs = (ag_s, ag_r) if x_like else (dy_s, dy_r)
        gathers[kind, u] = [
            send(src, buf.at[own], ss.at[u, 0], rs.at[u, 0], right),
            send(src, buf.at[own], ss.at[u, 1], rs.at[u, 1], left),
        ]

    def pass_on(kind, u):
        x_like = kind == "x"
        buf = xg.at[u] if x_like else dyg.at[u]
        ss, rs = (ag_s, ag_r) if x_like else (dy_s, dy_r)
        near = gathers[kind, u]
        near[0].wait_recv()
        first = buf.at[block_half(tensor_peer(3), 0)]
        on = [send(first, first, ss.at[u, 2], rs.at[u, 2], right)]
        near[1].wait_recv()
        second = buf.at[block_half(tensor_peer(1), 1)]
        on.append(send(second, second, ss.at[u, 3], rs.at[u, 3], left))
        gathers[kind, u] = on

    def gathered(kind, u):
        if (kind, u) in own_copies:
            own_copies[kind, u].wait()
        for copy in gathers[kind, u]:
            copy.wait_recv()

    def partner(chunk):
        return jnp.where(low_half, pltpu.roll(chunk, 96, 1), pltpu.roll(chunk, 32, 1))

    def forward(u):
        t, m = u // 2, u % 2
        x = xg[u].astype(F32)
        inverse = lax.rsqrt(jnp.mean(x * x, axis=-1, keepdims=True) + EPSILON)
        normed = (x * inverse * gain[m]).astype(BF16)
        for i in range(width // 256):
            n_t[u, i * 256 : (i + 1) * 256, :] = jnp.transpose(normed[:, i * 256 : (i + 1) * 256])
        projected = nn(normed, wq[m])
        for i in range(4):
            chunk = projected[:, i * 128 : (i + 1) * 128]
            q_rot[u, :, i * 128 : (i + 1) * 128] = (chunk * rope[0] + partner(chunk) * rope[1]).astype(BF16)
        chunk = projected[:, 512:640]
        both = (chunk * rope[2] + partner(chunk) * rope[3]).astype(BF16).astype(F32)
        key_low = jnp.where(first_head, both, 0.0)
        value_high = jnp.where(first_head, 0.0, both)
        kk[u, 0:128, :] = key_low.astype(BF16)
        kk[u, 128:256, :] = pltpu.roll(key_low, HD, 1).astype(BF16)
        vv[u, 0:128, :] = pltpu.roll(value_high, HD, 1).astype(BF16)
        vv[u, 128:256, :] = value_high.astype(BF16)
        causal = lax.broadcasted_iota(jnp.int32, (length, length), 0) >= lax.broadcasted_iota(
            jnp.int32, (length, length), 1
        )
        for i in range(4):
            scores = nt(q_rot[u, :, i * 128 : (i + 1) * 128], kk[u]) * SCALE
            low = []
            for h in range(2):
                part_scores = jnp.where(causal, scores[:, h * 128 : (h + 1) * 128], -1e30)
                e = jnp.exp(part_scores - jnp.max(part_scores, axis=-1, keepdims=True))
                p = e / jnp.sum(e, axis=-1, keepdims=True)
                prob[u, :, (2 * i + h) * 128 : (2 * i + h + 1) * 128] = p
                low.append(p.astype(BF16))
            att[m, t * 128 : (t + 1) * 128, i * 128 : (i + 1) * 128] = nn(
                jnp.concatenate(low, axis=1), vv[u]
            ).astype(BF16)

    def backward(u):
        t, m = u // 2, u % 2
        grad_att = nt(dyg[u], wo[m]).astype(BF16)
        acc_k = jnp.zeros((256, 128), F32)
        acc_v = jnp.zeros((256, 128), F32)
        slot = pl.ds(pl.multiple_of((z * 2 + t) * 128, 128), 128)
        for i in range(4):
            da = grad_att[:, i * 128 : (i + 1) * 128]
            grad_soft = nt(da, vv[u])
            low, grads = [], []
            for h in range(2):
                p = prob[u, :, (2 * i + h) * 128 : (2 * i + h + 1) * 128]
                g = grad_soft[:, h * 128 : (h + 1) * 128]
                total = jnp.sum(p * g, axis=-1, keepdims=True)
                grads.append((p * (g - total) * SCALE).astype(BF16))
                low.append(p.astype(BF16))
            grads = jnp.concatenate(grads, axis=1)
            low = jnp.concatenate(low, axis=1)
            gq = nn(grads, kk[u])
            gpr[m, slot, i * 128 : (i + 1) * 128] = (gq * rope[0] - partner(gq) * rope[1]).astype(BF16)
            acc_k = acc_k + tn(grads, q_rot[u, :, i * 128 : (i + 1) * 128])
            acc_v = acc_v + tn(low, da)
        grad_k = acc_k[0:128] + pltpu.roll(acc_k[128:256], HD, 1)
        grad_v = pltpu.roll(acc_v[0:128], HD, 1) + acc_v[128:256]
        both = jnp.where(first_head, grad_k, grad_v)
        gpr[m, slot, 512:640] = (both * rope[2] - partner(both) * rope[3]).astype(BF16)
        gp = gpr[m, slot, :]
        for i in range(width // 512):
            gn[u, :, i * 512 : (i + 1) * 512] = nt(gp, wq[m, i * 512 : (i + 1) * 512, :]).astype(BF16)

    scatters = {}

    def scatter(u):
        def out(slot, block, h, to):
            return send(gn.at[u, block_half(block, h)], rsr.at[u, slot], rs_s.at[u, slot], rs_r.at[u, slot], to)

        scatters[u] = {
            0: out(0, tensor_peer(2), 0, right),
            3: out(3, tensor_peer(2), 1, left),
            1: out(1, tensor_peer(1), 1, right),
            4: out(4, tensor_peer(3), 0, left),
        }

    def scatter_on(u):
        for i, slot, block, h, to in ((0, 0, tensor_peer(1), 0, right), (1, 3, tensor_peer(3), 1, left)):
            scatters[u].pop(slot).wait_recv()
            both = gn[u, block_half(block, h), :].astype(F32) + rsr[u, slot].astype(F32)
            way[u, i] = both.astype(BF16)
            scatters[u][2 + 3 * i] = send(
                way.at[u, i], rsr.at[u, 2 + 3 * i], rs_s.at[u, 2 + 3 * i], rs_r.at[u, 2 + 3 * i], to
            )

    def finish(u):
        t, m = u // 2, u % 2
        for copy in scatters[u].values():
            copy.wait_recv()
        total = gn[u, own, :].astype(F32) + jnp.concatenate(
            [
                rsr[u, 2].astype(F32) + rsr[u, 4].astype(F32),
                rsr[u, 1].astype(F32) + rsr[u, 5].astype(F32),
            ],
            axis=0,
        )
        x = xg[u, own, :].astype(F32)
        inverse = lax.rsqrt(jnp.mean(x * x, axis=-1, keepdims=True) + EPSILON)
        unit = x * inverse
        g = total * gain[m]
        result = dyg[u, own, :].astype(F32) + inverse * (g - unit * jnp.mean(g * unit, axis=-1, keepdims=True))
        ug[u] = result.astype(BF16)
        scale = jnp.sum(total * unit, axis=0, keepdims=True)
        if t == 0:
            gain_sum[m] = scale
        else:
            gain_sum[m] = gain_sum[m] + scale

    def shift_copy(m):
        step = 1 if m == 1 else -1
        return pltpu.make_async_remote_copy(
            src_ref=ug.at[m],
            dst_ref=dyg.at[2 + m, own],
            send_sem=sh_s.at[m],
            recv_sem=sh_r.at[m],
            device_id=(lax.rem(s + step + n_s, n_s), c, j),
            device_id_type=MESH,
        )

    def sends(m):
        return s < n_s - 1 if m == 1 else s > 0

    def receives(m):
        return s > 0 if m == 1 else s < n_s - 1

    top_copy = pltpu.make_async_copy(t_hbm, dyg.at[3, own], own_sem.at[6])
    turn_copy = pltpu.make_async_copy(ug.at[1], dyg.at[2, own], own_sem.at[7])

    def shift(m):
        pl.when(sends(m))(lambda: shift_copy(m).start())
        if m == 1:
            pl.when(s == 0)(lambda: top_copy.start())
            pl.when(s == n_s - 1)(lambda: turn_copy.start())

    def shifted(m):
        pl.when(receives(m))(lambda: shift_copy(m).wait_recv())
        pl.when(jnp.logical_not(receives(m)))(lambda: (top_copy if m == 1 else turn_copy).wait())

    normed_copies, grad_copies, part_copies, pair_copies = {}, {}, {}, {}
    own_normed = {}

    def rows_of(block, size):
        return pl.ds(pl.multiple_of(block * size, size), size)

    def spread_normed(u):
        t, m = u // 2, u % 2
        lanes = pl.ds(pl.multiple_of((z * 2 + t) * 128, 128), 128)
        own_normed[u] = []
        normed_copies[u] = []
        for b in range(2):
            copy = pltpu.make_async_copy(
                n_t.at[u, rows_of(b * 4 + z, slice_q)], n_tr.at[m, b, :, lanes], own_sem.at[8 + u * 2 + b]
            )
            copy.start()
            own_normed[u].append(copy)
        for k in z_order:
            for b in range(2):
                normed_copies[u].append(
                    send(
                        n_t.at[u, rows_of(b * 4 + z_peer(k), slice_q)],
                        n_tr.at[m, b, :, lanes],
                        nt_s.at[u, b, k - 1],
                        nt_r.at[u, b, k - 1],
                        at_z(k),
                    )
                )

    def spread_grad(u):
        t, m = u // 2, u % 2
        slot = pl.ds(pl.multiple_of((z * 2 + t) * 128, 128), 128)
        grad_copies[u] = [
            send(gpr.at[m, slot], gpr.at[m, slot], gp_s.at[u, k - 1], gp_r.at[u, k - 1], at_z(k))
            for k in z_order
        ]

    def pair_send(name, i, src, dst):
        pair_copies[name] = send(src, dst, pair_s.at[i], pair_r.at[i], pair)

    def share_attended(u):
        t, m = u // 2, u % 2
        mine = att.at[m, t * 128 : (t + 1) * 128]
        pair_send(("att", u), u, mine, att_far.at[m, t * 128 : (t + 1) * 128])

    def share_dy(u):
        pair_send(("dy", u), 4 + u, dyg.at[u, :, far_lanes], dy_far.at[u])

    def out_part(m):
        for u in (m, 2 + m):
            pair_copies["att", u].wait_recv()
            pair_copies["dy", u].wait_recv()
        lhs = jnp.concatenate([att[m], att_far[m]], axis=0)
        rhs = jnp.concatenate([dyg[m, :, half_lanes], dyg[2 + m, :, half_lanes], dy_far[m], dy_far[2 + m]], axis=0)
        for i in range(half // 256):
            part[m, :, i * 256 : (i + 1) * 256] = tn(lhs, rhs[:, i * 256 : (i + 1) * 256]).astype(BF16)

    def spread_out(m):
        part_copies[m] = []
        for k in z_order:
            for b in range(2):
                part_copies[m].append(
                    send(
                        part.at[m, rows_of(b * 4 + z_peer(k), slice_o)],
                        part_r.at[m, b, k - 1],
                        po_s.at[m, b, k - 1],
                        po_r.at[m, b, k - 1],
                        at_z(k),
                    )
                )

    def out_sum(m):
        for copy in part_copies[m]:
            copy.wait_recv()
        for b in (1 - y, y):
            total = part[m, rows_of(b * 4 + z, slice_o), :].astype(F32)
            for k in range(3):
                total = total + part_r[m, b, k].astype(F32)
            if b is y:
                go_v[m, :, half_lanes] = total.astype(BF16)
            else:
                go_far[m] = total.astype(BF16)
                pair_send(("out", m), 8 + m, go_far.at[m], go_v.at[m, :, half_lanes])

    def qkv_part(m):
        for u in (m, 2 + m):
            for copy in own_normed[u]:
                copy.wait()
            for copy in normed_copies[u] + grad_copies[u]:
                copy.wait_recv()
        wq_part[m] = nn(n_tr[m, 1 - y], gpr[m]).astype(BF16)
        pair_send(("wq", m), 10 + m, wq_part.at[m], wq_part_r.at[m])
        return nn(n_tr[m, y], gpr[m])

    gather("x", 1)
    gather("d", 1)
    pass_on("x", 1)
    gather("x", 0)
    pass_on("d", 1)
    gather("d", 0)

    loads["gain"].wait()
    loads["rope"].wait()
    gathered("x", 1)
    loads["wq1"].wait()
    forward(1)
    spread_normed(1)
    share_attended(1)
    pass_on("x", 0)
    gathered("d", 1)
    share_dy(1)
    loads["wo1"].wait()
    backward(1)
    scatter(1)
    pass_on("d", 0)
    spread_grad(1)
    gathered("x", 0)
    loads["wq0"].wait()
    forward(0)
    scatter_on(1)
    gather("x", 3)
    spread_normed(0)
    share_attended(0)
    gathered("d", 0)
    share_dy(0)
    loads["wo0"].wait()
    backward(0)
    scatter(0)
    spread_grad(0)
    finish(1)
    shift(1)
    pass_on("x", 3)
    scatter_on(0)
    gather("x", 2)
    finish(0)
    shift(0)
    gathered("x", 3)
    forward(3)
    share_attended(3)
    pass_on("x", 2)
    shifted(1)
    gather("d", 3)
    shifted(0)
    gather("d", 2)
    spread_normed(3)
    pass_on("d", 3)
    gathered("x", 2)
    forward(2)
    share_attended(2)
    spread_normed(2)
    pass_on("d", 2)
    gathered("d", 3)
    share_dy(3)
    backward(3)
    scatter(3)
    spread_grad(3)
    out_part(1)
    spread_out(1)
    scatter_on(3)
    gathered("d", 2)
    share_dy(2)
    backward(2)
    scatter(2)
    spread_grad(2)
    out_part(0)
    spread_out(0)
    scatter_on(2)
    outs = []

    def put(src, dst, i):
        outs.append(pltpu.make_async_copy(src, dst, out_sem.at[i]))
        outs[-1].start()

    gq_v[1] = qkv_part(1)
    finish(3)
    out_sum(1)
    finish(2)
    put(ug, ug_out, 0)

    g1[c] = gain_sum[...]
    first = [send(g1.at[c], g1.at[c], g1_s.at[k - 1], g1_r.at[k - 1], (s, tensor_peer(k), j)) for k in (1, 2, 3)]
    gq_v[0] = qkv_part(0)
    for copy in first:
        copy.wait_recv()
    g2[z] = ((g1[0] + g1[1]) + g1[2]) + g1[3]
    second = [send(g2.at[z], g2.at[z], g2_s.at[k - 1], g2_r.at[k - 1], at_z(k)) for k in (1, 2, 3)]
    out_sum(0)
    for copy in second:
        copy.wait_recv()
    g3[y] = ((g2[0] + g2[1]) + g2[2]) + g2[3]
    pair_send("gain", 12, g3.at[y], g3.at[y])
    for m in (1, 0):
        pair_copies["wq", m].wait_recv()
        gq_low[m] = (gq_v[m] + wq_part_r[m].astype(F32)).astype(BF16)
        put(gq_low.at[m], gq_out.at[m], 1 + m)
    for m in (1, 0):
        pair_copies["out", m].wait_recv()
        put(go_v.at[m], go_out.at[m], 3 + m)
    pair_copies["gain"].wait_recv()
    gg_v[...] = g3[0] + g3[1]
    put(gg_v, gg_out, 5)

    for m in (0, 1):
        pl.when(sends(m))(lambda m=m: shift_copy(m).wait_send())
    for copy in sent:
        copy.wait_send()
    for copy in outs:
        copy.wait()


def copy_out(*refs):
    n = len(refs) // 3
    srcs, dsts, held, sems = refs[:n], refs[n : 2 * n], refs[2 * n : 3 * n], refs[3 * n]
    inward = [pltpu.make_async_copy(srcs[i], held[i], sems.at[0, i]) for i in range(n)]
    outward = [pltpu.make_async_copy(held[i], dsts[i], sems.at[1, i]) for i in range(n)]
    for copy in inward:
        copy.start()
    for i in range(n):
        inward[i].wait()
        outward[i].start()
    for copy in outward:
        copy.wait()


def local(layer_in, carry_in, top_grad, w_qkv, w_out, gain):
    ticks, members = layer_in.shape[:2]
    rows, width = layer_in.shape[-2:]
    n_c, n_j = DIMS["tensor"], DIMS["dp"]
    length = rows * n_c
    units = ticks * members
    x = layer_in.reshape(units, rows, width)
    carry = carry_in.reshape(members, rows, width)
    top = top_grad.reshape(rows, width)
    wq = w_qkv[:, 0]
    wo = w_out[:, 0]
    cols, heads = wq.shape[2], wo.shape[1]
    slice_q, slice_o = width // n_j, heads // n_j
    tokens = 4 * ticks * length
    hbm = pl.BlockSpec(memory_space=pl.ANY)
    dma = pltpu.SemaphoreType.DMA
    outs = pl.pallas_call(
        kernel,
        out_shape=(
            jax.ShapeDtypeStruct((units, rows, width), BF16),
            jax.ShapeDtypeStruct((members, slice_q, cols), BF16),
            jax.ShapeDtypeStruct((members, slice_o, width), BF16),
            jax.ShapeDtypeStruct((members, 1, width), F32),
        ),
        in_specs=[hbm] * 7,
        out_specs=(hbm,) * 4,
        scratch_shapes=[
            pltpu.VMEM((members, width, cols), BF16),
            pltpu.VMEM((members, heads, width), BF16),
            pltpu.VMEM((members, 1, width), F32),
            pltpu.VMEM((4, length, 128), F32),
            pltpu.VMEM((units, length, width), BF16),
            pltpu.VMEM((units, length, width), BF16),
            pltpu.VMEM((units, width, length), BF16),
            pltpu.VMEM((members, 2, slice_q, tokens), BF16),
            pltpu.VMEM((members, tokens, cols), BF16),
            pltpu.VMEM((units, length, heads), BF16),
            pltpu.VMEM((units, 256, 128), BF16),
            pltpu.VMEM((units, 256, 128), BF16),
            pltpu.VMEM((units, length, GROUP * 128), F32),
            pltpu.VMEM((members, ticks * length, heads), BF16),
            pltpu.VMEM((units, length, width), BF16),
            pltpu.VMEM((units, 6, rows // 2, width), BF16),
            pltpu.VMEM((units, 2, rows // 2, width), BF16),
            pltpu.VMEM((units, rows, width), BF16),
            pltpu.VMEM((units, length, width // 2), BF16),
            pltpu.VMEM((members, ticks * length, heads), BF16),
            pltpu.VMEM((members, heads, width // 2), BF16),
            pltpu.VMEM((members, 2, 3, slice_o, width // 2), BF16),
            pltpu.VMEM((members, slice_q, cols), BF16),
            pltpu.VMEM((members, slice_q, cols), BF16),
            pltpu.VMEM((members, 1, width), F32),
            pltpu.VMEM((n_c, members, 1, width), F32),
            pltpu.VMEM((4, members, 1, width), F32),
            pltpu.VMEM((2, members, 1, width), F32),
            pltpu.VMEM((members, slice_q, cols), F32),
            pltpu.VMEM((members, slice_q, cols), BF16),
            pltpu.VMEM((members, slice_o, width), BF16),
            pltpu.VMEM((members, slice_o, width // 2), BF16),
            pltpu.VMEM((members, 1, width), F32),
            dma((6,)), dma((16,)), dma((6,)),
            dma((4, 4)), dma((4, 4)), dma((4, 4)), dma((4, 4)), dma((4, 6)), dma((4, 6)), dma((2,)), dma((2,)),
            dma((4, 2, 3)), dma((4, 2, 3)), dma((4, 3)), dma((4, 3)), dma((13,)), dma((13,)),
            dma((2, 2, 3)), dma((2, 2, 3)), dma((3,)), dma((3,)), dma((3,)), dma((3,)),
        ],
        compiler_params=pltpu.CompilerParams(has_side_effects=True, collective_id=0, vmem_limit_bytes=63 * 1024 * 1024),
    )(x, carry, top, wq, wo, gain, jnp.asarray(rope_tables(length)))
    unit_grads, grad_qkv, grad_out, grad_gain = pl.pallas_call(
        copy_out,
        out_shape=tuple(jax.ShapeDtypeStruct(o.shape, o.dtype) for o in outs),
        in_specs=[hbm] * 4,
        out_specs=(hbm,) * 4,
        scratch_shapes=[pltpu.VMEM(o.shape, o.dtype) for o in outs] + [dma((2, 4))],
    )(*outs)
    return (
        unit_grads.reshape(ticks, members, 1, 1, rows, width),
        grad_qkv[:, None],
        grad_out[:, None],
        grad_gain,
    )


def solution(mesh):
    in_specs = (
        P(None, None, "section", "dp", "tensor", None),
        P(None, "section", "dp", "tensor", None),
        P(None, "dp", "tensor", None),
        P(None, "section", None, "tensor"),
        P(None, "section", "tensor", None),
        P(None, "section", None),
    )
    out_specs = (
        P(None, None, "section", "dp", "tensor", None),
        P(None, "section", "dp", "tensor"),
        P(None, "section", ("tensor", "dp"), None),
        P(None, "section", None),
    )
    return jax.shard_map(local, mesh=mesh, in_specs=in_specs, out_specs=out_specs, check_vma=False)
```

```python
import functools
import math

import jax
import jax.numpy as jnp
import numpy as np
from jax import lax
from jax.experimental import pallas as pl
from jax.experimental.pallas import tpu as pltpu
from jax.sharding import PartitionSpec as P

HD = 64
GROUP = 8
EPSILON = 1e-06
ROPE_BASE = 1000000.0
SCALE = 1.0 / math.sqrt(HD)
F32 = jnp.float32
BF16 = jnp.bfloat16
MESH = pl.DeviceIdType.MESH
DIMS = dict(ticks=2, sections=4, tensor=4, dp=8)


def rope_tables(length):
    half = HD // 2
    exponent = np.arange(half, dtype=np.float32) * np.float32(2.0 / HD)
    frequency = np.power(np.float32(ROPE_BASE), -exponent).astype(np.float32)
    angle = np.arange(length, dtype=np.float32)[:, None] * frequency[None, :]
    cosine, sine = np.cos(angle), np.sin(angle)
    head_cos = np.concatenate([cosine, cosine], axis=1)
    head_sin = np.concatenate([-sine, sine], axis=1)
    return np.stack(
        [
            np.concatenate([head_cos, head_cos], axis=1),
            np.concatenate([head_sin, head_sin], axis=1),
            np.concatenate([head_cos, np.ones_like(head_cos)], axis=1),
            np.concatenate([head_sin, np.zeros_like(head_sin)], axis=1),
        ]
    ).astype(np.float32)


def nt(a, b):
    return lax.dot_general(a, b, (((1,), (1,)), ((), ())), preferred_element_type=F32)


def tn(a, b):
    return lax.dot_general(a, b, (((0,), (0,)), ((), ())), preferred_element_type=F32)


def nn(a, b):
    return jnp.dot(a, b, preferred_element_type=F32)


def kernel(
    x_hbm, c_hbm, t_hbm, wq_hbm, wo_hbm, gain_hbm, rope_hbm,
    ug_out, gq_out, go_out, gg_out,
    wq, wo, gain, rope, xg, dyg, norm_rows, n_t, n_tr, gpr, q_rot, kk, vv, prob, att, gn, rsr, way, ug,
    dy_far, att_far, part, part_r, part_way, wq_part, wq_part_r, gain_sum, g1, g2, g3, gq_v, gq_low, go_v, go_far, gg_v,
    w_sem, own_sem, out_sem, ag_s, ag_r, dy_s, dy_r, rs_s, rs_r, sh_s, sh_r,
    nt_s, nt_r, gp_s, gp_r, pair_s, pair_r, po_s, po_r, g1_s, g1_r, g2_s, g2_r,
):
    s, c, j = lax.axis_index("section"), lax.axis_index("tensor"), lax.axis_index("dp")
    n_s, n_c, n_j = DIMS["sections"], DIMS["tensor"], DIMS["dp"]
    rows = x_hbm.shape[1]
    length = rows * n_c
    width = x_hbm.shape[2]
    slice_q = gq_out.shape[1]
    slice_o = go_out.shape[1]
    own = pl.ds(pl.multiple_of(c * rows, rows), rows)
    lane = lax.broadcasted_iota(jnp.int32, (length, 128), 1)
    low_half = (lane % HD) < (HD // 2)
    first_head = lane < HD

    def tensor_peer(k):
        return lax.rem(c + k, n_c)

    z, y = lax.rem(j, 4), lax.div(j, 4)
    far = (1 - y) * 4 + z
    half = width // 2
    half_lanes = pl.ds(pl.multiple_of(y * half, half), half)
    far_lanes = pl.ds(pl.multiple_of((1 - y) * half, half), half)

    def z_peer(k):
        return lax.rem(z + k, 4)

    def at_z(k):
        return (s, c, y * 4 + z_peer(k))

    pair = (s, c, far)
    z_order = (1, 3, 2)

    sent = []

    def send(src, dst, s_sem, r_sem, to):
        copy = pltpu.make_async_remote_copy(
            src_ref=src, dst_ref=dst, send_sem=s_sem, recv_sem=r_sem, device_id=to, device_id_type=MESH
        )
        copy.start()
        sent.append(copy)
        return copy

    loads = {}

    def load(name, src, dst, i):
        loads[name] = pltpu.make_async_copy(src, dst, w_sem.at[i])
        loads[name].start()

    load("gain", gain_hbm, gain, 0)
    load("rope", rope_hbm, rope, 1)
    own_copies = {}
    for i, (name, src, dst) in enumerate(
        [(("x", u), x_hbm.at[u], xg.at[u, own]) for u in range(4)]
        + [(("d", u), c_hbm.at[u], dyg.at[u, own]) for u in range(2)]
    ):
        own_copies[name] = pltpu.make_async_copy(src, dst, own_sem.at[i])
        own_copies[name].start()
    barrier = pltpu.get_barrier_semaphore()
    friends = [(s, tensor_peer(k), j) for k in (1, 2, 3)] + [at_z(k) for k in (1, 2, 3)]
    friends += [pair, (lax.rem(s + 1, n_s), c, j), (lax.rem(s + n_s - 1, n_s), c, j)]
    for friend in friends:
        pl.semaphore_signal(barrier, inc=1, device_id=friend, device_id_type=MESH)
    load("wq1", wq_hbm.at[1], wq.at[1], 2)
    load("wo1", wo_hbm.at[1], wo.at[1], 3)
    load("wq0", wq_hbm.at[0], wq.at[0], 4)
    load("wo0", wo_hbm.at[0], wo.at[0], 5)

    pl.semaphore_wait(barrier, len(friends))

    half_rows = rows // 2
    right, left = (s, tensor_peer(1), j), (s, tensor_peer(3), j)
    gathers = {}

    def block_half(block, h):
        return pl.ds(pl.multiple_of(block * rows + h * half_rows, half_rows), half_rows)

    def gather(kind, u):
        x_like = kind == "x"
        buf = xg.at[u] if x_like else dyg.at[u]
        src = x_hbm.at[u] if x_like else c_hbm.at[u] if u < 2 else dyg.at[u, own]
        ss, rs = (ag_s, ag_r) if x_like else (dy_s, dy_r)
        gathers[kind, u] = [
            send(src, buf.at[own], ss.at[u, 0], rs.at[u, 0], right),
            send(src, buf.at[own], ss.at[u, 1], rs.at[u, 1], left),
        ]

    def pass_on(kind, u):
        x_like = kind == "x"
        buf = xg.at[u] if x_like else dyg.at[u]
        ss, rs = (ag_s, ag_r) if x_like else (dy_s, dy_r)
        near = gathers[kind, u]
        near[0].wait_recv()
        first = buf.at[block_half(tensor_peer(3), 0)]
        on = [send(first, first, ss.at[u, 2], rs.at[u, 2], right)]
        near[1].wait_recv()
        second = buf.at[block_half(tensor_peer(1), 1)]
        on.append(send(second, second, ss.at[u, 3], rs.at[u, 3], left))
        gathers[kind, u] = on

    def gathered(kind, u):
        if (kind, u) in own_copies:
            own_copies[kind, u].wait()
        for copy in gathers[kind, u]:
            copy.wait_recv()

    def partner(chunk):
        return jnp.where(low_half, pltpu.roll(chunk, 96, 1), pltpu.roll(chunk, 32, 1))

    def normalize(u):
        m = u % 2
        x = xg[u].astype(F32)
        inverse = lax.rsqrt(jnp.mean(x * x, axis=-1, keepdims=True) + EPSILON)
        normed = (x * inverse * gain[m]).astype(BF16)
        for i in range(width // 256):
            n_t[u, i * 256 : (i + 1) * 256, :] = jnp.transpose(normed[:, i * 256 : (i + 1) * 256])
        norm_rows[u % 2] = normed

    def forward(u):
        t, m = u // 2, u % 2
        projected = nn(norm_rows[u % 2], wq[m])
        for i in range(4):
            chunk = projected[:, i * 128 : (i + 1) * 128]
            q_rot[u, :, i * 128 : (i + 1) * 128] = (chunk * rope[0] + partner(chunk) * rope[1]).astype(BF16)
        chunk = projected[:, 512:640]
        both = (chunk * rope[2] + partner(chunk) * rope[3]).astype(BF16).astype(F32)
        key_low = jnp.where(first_head, both, 0.0)
        value_high = jnp.where(first_head, 0.0, both)
        kk[u, 0:128, :] = key_low.astype(BF16)
        kk[u, 128:256, :] = pltpu.roll(key_low, HD, 1).astype(BF16)
        vv[u, 0:128, :] = pltpu.roll(value_high, HD, 1).astype(BF16)
        vv[u, 128:256, :] = value_high.astype(BF16)
        causal = lax.broadcasted_iota(jnp.int32, (length, length), 0) >= lax.broadcasted_iota(
            jnp.int32, (length, length), 1
        )
        for i in range(4):
            scores = nt(q_rot[u, :, i * 128 : (i + 1) * 128], kk[u]) * SCALE
            low = []
            for h in range(2):
                part_scores = jnp.where(causal, scores[:, h * 128 : (h + 1) * 128], -1e30)
                e = jnp.exp(part_scores - jnp.max(part_scores, axis=-1, keepdims=True))
                p = e / jnp.sum(e, axis=-1, keepdims=True)
                prob[u, :, (2 * i + h) * 128 : (2 * i + h + 1) * 128] = p
                low.append(p.astype(BF16))
            att[m, t * 128 : (t + 1) * 128, i * 128 : (i + 1) * 128] = nn(
                jnp.concatenate(low, axis=1), vv[u]
            ).astype(BF16)

    def backward(u):
        t, m = u // 2, u % 2
        grad_att = nt(dyg[u], wo[m]).astype(BF16)
        acc_k = jnp.zeros((256, 128), F32)
        acc_v = jnp.zeros((256, 128), F32)
        slot = pl.ds(pl.multiple_of((z * 2 + t) * 128, 128), 128)
        for i in range(4):
            da = grad_att[:, i * 128 : (i + 1) * 128]
            grad_soft = nt(da, vv[u])
            low, grads = [], []
            for h in range(2):
                p = prob[u, :, (2 * i + h) * 128 : (2 * i + h + 1) * 128]
                g = grad_soft[:, h * 128 : (h + 1) * 128]
                total = jnp.sum(p * g, axis=-1, keepdims=True)
                grads.append((p * (g - total) * SCALE).astype(BF16))
                low.append(p.astype(BF16))
            grads = jnp.concatenate(grads, axis=1)
            low = jnp.concatenate(low, axis=1)
            gq = nn(grads, kk[u])
            gpr[m, slot, i * 128 : (i + 1) * 128] = (gq * rope[0] - partner(gq) * rope[1]).astype(BF16)
            acc_k = acc_k + tn(grads, q_rot[u, :, i * 128 : (i + 1) * 128])
            acc_v = acc_v + tn(low, da)
        grad_k = acc_k[0:128] + pltpu.roll(acc_k[128:256], HD, 1)
        grad_v = pltpu.roll(acc_v[0:128], HD, 1) + acc_v[128:256]
        both = jnp.where(first_head, grad_k, grad_v)
        gpr[m, slot, 512:640] = (both * rope[2] - partner(both) * rope[3]).astype(BF16)
        gp = gpr[m, slot, :]
        for i in range(width // 512):
            gn[u, :, i * 512 : (i + 1) * 512] = nt(gp, wq[m, i * 512 : (i + 1) * 512, :]).astype(BF16)

    scatters = {}

    def scatter(u):
        def out(slot, block, h, to):
            return send(gn.at[u, block_half(block, h)], rsr.at[u, slot], rs_s.at[u, slot], rs_r.at[u, slot], to)

        scatters[u] = {
            0: out(0, tensor_peer(2), 0, right),
            3: out(3, tensor_peer(2), 1, left),
            1: out(1, tensor_peer(1), 1, right),
            4: out(4, tensor_peer(3), 0, left),
        }

    def scatter_on(u):
        for i, slot, block, h, to in ((0, 0, tensor_peer(1), 0, right), (1, 3, tensor_peer(3), 1, left)):
            scatters[u].pop(slot).wait_recv()
            both = gn[u, block_half(block, h), :].astype(F32) + rsr[u, slot].astype(F32)
            way[u, i] = both.astype(BF16)
            scatters[u][2 + 3 * i] = send(
                way.at[u, i], rsr.at[u, 2 + 3 * i], rs_s.at[u, 2 + 3 * i], rs_r.at[u, 2 + 3 * i], to
            )

    def finish(u):
        t, m = u // 2, u % 2
        for copy in scatters[u].values():
            copy.wait_recv()
        total = gn[u, own, :].astype(F32) + jnp.concatenate(
            [
                rsr[u, 2].astype(F32) + rsr[u, 4].astype(F32),
                rsr[u, 1].astype(F32) + rsr[u, 5].astype(F32),
            ],
            axis=0,
        )
        x = xg[u, own, :].astype(F32)
        inverse = lax.rsqrt(jnp.mean(x * x, axis=-1, keepdims=True) + EPSILON)
        unit = x * inverse
        g = total * gain[m]
        result = dyg[u, own, :].astype(F32) + inverse * (g - unit * jnp.mean(g * unit, axis=-1, keepdims=True))
        ug[u] = result.astype(BF16)
        scale = jnp.sum(total * unit, axis=0, keepdims=True)
        if t == 0:
            gain_sum[m] = scale
        else:
            gain_sum[m] = gain_sum[m] + scale

    def shift_copy(m):
        step = 1 if m == 1 else -1
        return pltpu.make_async_remote_copy(
            src_ref=ug.at[m],
            dst_ref=dyg.at[2 + m, own],
            send_sem=sh_s.at[m],
            recv_sem=sh_r.at[m],
            device_id=(lax.rem(s + step + n_s, n_s), c, j),
            device_id_type=MESH,
        )

    def sends(m):
        return s < n_s - 1 if m == 1 else s > 0

    def receives(m):
        return s > 0 if m == 1 else s < n_s - 1

    top_copy = pltpu.make_async_copy(t_hbm, dyg.at[3, own], own_sem.at[6])
    turn_copy = pltpu.make_async_copy(ug.at[1], dyg.at[2, own], own_sem.at[7])

    def shift(m):
        pl.when(sends(m))(lambda: shift_copy(m).start())
        if m == 1:
            pl.when(s == 0)(lambda: top_copy.start())
            pl.when(s == n_s - 1)(lambda: turn_copy.start())

    def shifted(m):
        pl.when(receives(m))(lambda: shift_copy(m).wait_recv())
        pl.when(jnp.logical_not(receives(m)))(lambda: (top_copy if m == 1 else turn_copy).wait())

    normed_copies, grad_copies, part_copies, pair_copies = {}, {}, {}, {}
    own_normed = {}

    def rows_of(block, size):
        return pl.ds(pl.multiple_of(block * size, size), size)

    def spread_normed(u):
        t, m = u // 2, u % 2
        lanes = pl.ds(pl.multiple_of((z * 2 + t) * 128, 128), 128)
        own_normed[u] = []
        normed_copies[u] = []
        for b in range(2):
            copy = pltpu.make_async_copy(
                n_t.at[u, rows_of(b * 4 + z, slice_q)], n_tr.at[m, b, :, lanes], own_sem.at[8 + u * 2 + b]
            )
            copy.start()
            own_normed[u].append(copy)
        for k in z_order:
            for b in range(2):
                normed_copies[u].append(
                    send(
                        n_t.at[u, rows_of(b * 4 + z_peer(k), slice_q)],
                        n_tr.at[m, b, :, lanes],
                        nt_s.at[u, b, k - 1],
                        nt_r.at[u, b, k - 1],
                        at_z(k),
                    )
                )

    def tokens_of(block, t, h=None):
        start = (block * 2 + t) * 128
        if h is None:
            return pl.ds(pl.multiple_of(start, 128), 128)
        return pl.ds(pl.multiple_of(start + h * 64, 64), 64)

    def spread_grad(u):
        t, m = u // 2, u % 2
        mine = gpr.at[m, tokens_of(z, t)]
        grad_copies[u] = [
            send(mine, mine, gp_s.at[u, 0], gp_r.at[u, 0], at_z(1)),
            send(mine, mine, gp_s.at[u, 1], gp_r.at[u, 1], at_z(3)),
        ]

    def spread_grad_on(u):
        t, m = u // 2, u % 2
        near = grad_copies[u]
        near[0].wait_recv()
        first = gpr.at[m, tokens_of(z_peer(3), t, 0)]
        on = [send(first, first, gp_s.at[u, 2], gp_r.at[u, 2], at_z(1))]
        near[1].wait_recv()
        second = gpr.at[m, tokens_of(z_peer(1), t, 1)]
        on.append(send(second, second, gp_s.at[u, 3], gp_r.at[u, 3], at_z(3)))
        grad_copies[u] = on

    def pair_send(name, i, src, dst):
        pair_copies[name] = send(src, dst, pair_s.at[i], pair_r.at[i], pair)

    def share_attended(u):
        t, m = u // 2, u % 2
        mine = att.at[m, t * 128 : (t + 1) * 128]
        pair_send(("att", u), u, mine, att_far.at[m, t * 128 : (t + 1) * 128])

    def share_dy(u):
        pair_send(("dy", u), 4 + u, dyg.at[u, :, far_lanes], dy_far.at[u])

    def out_part(m):
        for u in (m, 2 + m):
            pair_copies["att", u].wait_recv()
            pair_copies["dy", u].wait_recv()
        lhs = jnp.concatenate([att[m], att_far[m]], axis=0)
        rhs = jnp.concatenate([dyg[m, :, half_lanes], dyg[2 + m, :, half_lanes], dy_far[m], dy_far[2 + m]], axis=0)
        for i in range(half // 256):
            part[m, :, i * 256 : (i + 1) * 256] = tn(lhs, rhs[:, i * 256 : (i + 1) * 256]).astype(BF16)

    def spread_out(m):
        def out(slot, block, b, to):
            src = part.at[m, rows_of(b * 4 + block, slice_o)]
            return send(src, part_r.at[m, slot], po_s.at[m, slot], po_r.at[m, slot], to)

        part_copies[m] = {
            0: out(0, z_peer(2), 0, at_z(1)),
            3: out(3, z_peer(2), 1, at_z(3)),
            1: out(1, z_peer(1), 1, at_z(1)),
            4: out(4, z_peer(3), 0, at_z(3)),
        }

    def spread_out_on(m):
        for i, slot, block, b, to in ((0, 0, z_peer(1), 0, at_z(1)), (1, 3, z_peer(3), 1, at_z(3))):
            part_copies[m].pop(slot).wait_recv()
            both = part[m, rows_of(b * 4 + block, slice_o), :].astype(F32) + part_r[m, slot].astype(F32)
            part_way[m, i] = both.astype(BF16)
            last = 2 + 3 * i
            part_copies[m][last] = send(
                part_way.at[m, i], part_r.at[m, last], po_s.at[m, last], po_r.at[m, last], to
            )

    def out_sum(m):
        for copy in part_copies[m].values():
            copy.wait_recv()
        totals = []
        for b, slots in ((0, (2, 4)), (1, (1, 5))):
            total = part[m, rows_of(b * 4 + z, slice_o), :].astype(F32)
            for slot in slots:
                total = total + part_r[m, slot].astype(F32)
            totals.append(total.astype(BF16))
        go_v[m, :, half_lanes] = jnp.where(y == 0, totals[0], totals[1])
        go_far[m] = jnp.where(y == 0, totals[1], totals[0])
        pair_send(("out", m), 8 + m, go_far.at[m], go_v.at[m, :, half_lanes])

    def qkv_part(m):
        for u in (m, 2 + m):
            for copy in own_normed[u]:
                copy.wait()
            for copy in normed_copies[u] + grad_copies[u]:
                copy.wait_recv()
        wq_part[m] = nn(n_tr[m, 1 - y], gpr[m]).astype(BF16)
        pair_send(("wq", m), 10 + m, wq_part.at[m], wq_part_r.at[m])
        return nn(n_tr[m, y], gpr[m])

    gather("x", 1)
    gather("d", 1)
    pass_on("x", 1)
    gather("x", 0)
    pass_on("d", 1)
    gather("d", 0)

    loads["gain"].wait()
    loads["rope"].wait()
    gathered("x", 1)
    normalize(1)
    spread_normed(1)
    loads["wq1"].wait()
    forward(1)
    share_attended(1)
    pass_on("x", 0)
    gathered("d", 1)
    share_dy(1)
    loads["wo1"].wait()
    backward(1)
    scatter(1)
    spread_grad(1)
    pass_on("d", 0)
    gathered("x", 0)
    normalize(0)
    spread_normed(0)
    scatter_on(1)
    gather("x", 3)
    loads["wq0"].wait()
    forward(0)
    share_attended(0)
    gathered("d", 0)
    share_dy(0)
    loads["wo0"].wait()
    backward(0)
    scatter(0)
    spread_grad_on(1)
    spread_grad(0)
    finish(1)
    shift(1)
    pass_on("x", 3)
    scatter_on(0)
    gather("x", 2)
    gathered("x", 3)
    normalize(3)
    spread_normed(3)
    finish(0)
    shift(0)
    forward(3)
    share_attended(3)
    shifted(1)
    gather("d", 3)
    pass_on("x", 2)
    shifted(0)
    gather("d", 2)
    spread_grad_on(0)
    pass_on("d", 3)
    gathered("x", 2)
    normalize(2)
    spread_normed(2)
    forward(2)
    share_attended(2)
    pass_on("d", 2)
    gathered("d", 3)
    share_dy(3)
    backward(3)
    scatter(3)
    spread_grad(3)
    gathered("d", 2)
    share_dy(2)
    backward(2)
    scatter(2)
    spread_grad(2)
    scatter_on(3)
    spread_grad_on(3)
    out_part(1)
    spread_out(1)
    scatter_on(2)
    spread_grad_on(2)
    out_part(0)
    spread_out(0)
    outs = []

    def put(src, dst, i):
        outs.append(pltpu.make_async_copy(src, dst, out_sem.at[i]))
        outs[-1].start()

    gq_v[1] = qkv_part(1)
    spread_out_on(1)
    gq_v[0] = qkv_part(0)
    spread_out_on(0)
    finish(3)
    finish(2)
    put(ug, ug_out, 0)

    g1[c] = gain_sum[...]
    first = [send(g1.at[c], g1.at[c], g1_s.at[k - 1], g1_r.at[k - 1], (s, tensor_peer(k), j)) for k in (1, 2, 3)]
    for copy in first:
        copy.wait_recv()
    g2[z] = ((g1[0] + g1[1]) + g1[2]) + g1[3]
    second = [send(g2.at[z], g2.at[z], g2_s.at[k - 1], g2_r.at[k - 1], at_z(k)) for k in (1, 2, 3)]
    out_sum(1)
    for copy in second:
        copy.wait_recv()
    g3[y] = ((g2[0] + g2[1]) + g2[2]) + g2[3]
    pair_send("gain", 12, g3.at[y], g3.at[y])
    def put_qkv(m):
        pair_copies["wq", m].wait_recv()
        gq_low[m] = (gq_v[m] + wq_part_r[m].astype(F32)).astype(BF16)
        put(gq_low.at[m], gq_out.at[m], 1 + m)

    put_qkv(1)
    out_sum(0)
    put_qkv(0)
    for m in (1, 0):
        pair_copies["out", m].wait_recv()
        put(go_v.at[m], go_out.at[m], 3 + m)
    pair_copies["gain"].wait_recv()
    gg_v[...] = g3[0] + g3[1]
    put(gg_v, gg_out, 5)

    for m in (0, 1):
        pl.when(sends(m))(lambda m=m: shift_copy(m).wait_send())
    for copy in sent:
        copy.wait_send()
    for copy in outs:
        copy.wait()


def copy_out(*refs):
    n = len(refs) // 3
    srcs, dsts, held, sems = refs[:n], refs[n : 2 * n], refs[2 * n : 3 * n], refs[3 * n]
    inward = [pltpu.make_async_copy(srcs[i], held[i], sems.at[0, i]) for i in range(n)]
    outward = [pltpu.make_async_copy(held[i], dsts[i], sems.at[1, i]) for i in range(n)]
    for copy in inward:
        copy.start()
    for i in range(n):
        inward[i].wait()
        outward[i].start()
    for copy in outward:
        copy.wait()


def local(layer_in, carry_in, top_grad, w_qkv, w_out, gain):
    ticks, members = layer_in.shape[:2]
    rows, width = layer_in.shape[-2:]
    n_c, n_j = DIMS["tensor"], DIMS["dp"]
    length = rows * n_c
    units = ticks * members
    x = layer_in.reshape(units, rows, width)
    carry = carry_in.reshape(members, rows, width)
    top = top_grad.reshape(rows, width)
    wq = w_qkv[:, 0]
    wo = w_out[:, 0]
    cols, heads = wq.shape[2], wo.shape[1]
    slice_q, slice_o = width // n_j, heads // n_j
    tokens = 4 * ticks * length
    hbm = pl.BlockSpec(memory_space=pl.ANY)
    dma = pltpu.SemaphoreType.DMA
    outs = pl.pallas_call(
        kernel,
        out_shape=(
            jax.ShapeDtypeStruct((units, rows, width), BF16),
            jax.ShapeDtypeStruct((members, slice_q, cols), BF16),
            jax.ShapeDtypeStruct((members, slice_o, width), BF16),
            jax.ShapeDtypeStruct((members, 1, width), F32),
        ),
        in_specs=[hbm] * 7,
        out_specs=(hbm,) * 4,
        scratch_shapes=[
            pltpu.VMEM((members, width, cols), BF16),
            pltpu.VMEM((members, heads, width), BF16),
            pltpu.VMEM((members, 1, width), F32),
            pltpu.VMEM((4, length, 128), F32),
            pltpu.VMEM((units, length, width), BF16),
            pltpu.VMEM((units, length, width), BF16),
            pltpu.VMEM((members, length, width), BF16),
            pltpu.VMEM((units, width, length), BF16),
            pltpu.VMEM((members, 2, slice_q, tokens), BF16),
            pltpu.VMEM((members, tokens, cols), BF16),
            pltpu.VMEM((units, length, heads), BF16),
            pltpu.VMEM((units, 256, 128), BF16),
            pltpu.VMEM((units, 256, 128), BF16),
            pltpu.VMEM((units, length, GROUP * 128), F32),
            pltpu.VMEM((members, ticks * length, heads), BF16),
            pltpu.VMEM((units, length, width), BF16),
            pltpu.VMEM((units, 6, rows // 2, width), BF16),
            pltpu.VMEM((units, 2, rows // 2, width), BF16),
            pltpu.VMEM((units, rows, width), BF16),
            pltpu.VMEM((units, length, width // 2), BF16),
            pltpu.VMEM((members, ticks * length, heads), BF16),
            pltpu.VMEM((members, heads, width // 2), BF16),
            pltpu.VMEM((members, 6, slice_o, width // 2), BF16),
            pltpu.VMEM((members, 2, slice_o, width // 2), BF16),
            pltpu.VMEM((members, slice_q, cols), BF16),
            pltpu.VMEM((members, slice_q, cols), BF16),
            pltpu.VMEM((members, 1, width), F32),
            pltpu.VMEM((n_c, members, 1, width), F32),
            pltpu.VMEM((4, members, 1, width), F32),
            pltpu.VMEM((2, members, 1, width), F32),
            pltpu.VMEM((members, slice_q, cols), F32),
            pltpu.VMEM((members, slice_q, cols), BF16),
            pltpu.VMEM((members, slice_o, width), BF16),
            pltpu.VMEM((members, slice_o, width // 2), BF16),
            pltpu.VMEM((members, 1, width), F32),
            dma((6,)), dma((16,)), dma((6,)),
            dma((4, 4)), dma((4, 4)), dma((4, 4)), dma((4, 4)), dma((4, 6)), dma((4, 6)), dma((2,)), dma((2,)),
            dma((4, 2, 3)), dma((4, 2, 3)), dma((4, 4)), dma((4, 4)), dma((13,)), dma((13,)),
            dma((2, 6)), dma((2, 6)), dma((3,)), dma((3,)), dma((3,)), dma((3,)),
        ],
        compiler_params=pltpu.CompilerParams(has_side_effects=True, collective_id=0, vmem_limit_bytes=63 * 1024 * 1024),
    )(x, carry, top, wq, wo, gain, jnp.asarray(rope_tables(length)))
    unit_grads, grad_qkv, grad_out, grad_gain = pl.pallas_call(
        copy_out,
        out_shape=tuple(jax.ShapeDtypeStruct(o.shape, o.dtype) for o in outs),
        in_specs=[hbm] * 4,
        out_specs=(hbm,) * 4,
        scratch_shapes=[pltpu.VMEM(o.shape, o.dtype) for o in outs] + [dma((2, 4))],
    )(*outs)
    return (
        unit_grads.reshape(ticks, members, 1, 1, rows, width),
        grad_qkv[:, None],
        grad_out[:, None],
        grad_gain,
    )


def solution(mesh):
    in_specs = (
        P(None, None, "section", "dp", "tensor", None),
        P(None, "section", "dp", "tensor", None),
        P(None, "dp", "tensor", None),
        P(None, "section", None, "tensor"),
        P(None, "section", "tensor", None),
        P(None, "section", None),
    )
    out_specs = (
        P(None, None, "section", "dp", "tensor", None),
        P(None, "section", "dp", "tensor"),
        P(None, "section", ("tensor", "dp"), None),
        P(None, "section", None),
    )
    return jax.shard_map(local, mesh=mesh, in_specs=in_specs, out_specs=out_specs, check_vma=False)
```

```python
import functools
import math

import jax
import jax.numpy as jnp
import numpy as np
from jax import lax
from jax.experimental import pallas as pl
from jax.experimental.pallas import tpu as pltpu
from jax.sharding import PartitionSpec as P

HD = 64
GROUP = 8
EPSILON = 1e-06
ROPE_BASE = 1000000.0
SCALE = 1.0 / math.sqrt(HD)
F32 = jnp.float32
BF16 = jnp.bfloat16
MESH = pl.DeviceIdType.MESH
DIMS = dict(ticks=2, sections=4, tensor=4, dp=8)


def rope_tables(length):
    half = HD // 2
    exponent = np.arange(half, dtype=np.float32) * np.float32(2.0 / HD)
    frequency = np.power(np.float32(ROPE_BASE), -exponent).astype(np.float32)
    angle = np.arange(length, dtype=np.float32)[:, None] * frequency[None, :]
    cosine, sine = np.cos(angle), np.sin(angle)
    head_cos = np.concatenate([cosine, cosine], axis=1)
    head_sin = np.concatenate([-sine, sine], axis=1)
    return np.stack(
        [
            np.concatenate([head_cos, head_cos], axis=1),
            np.concatenate([head_sin, head_sin], axis=1),
            np.concatenate([head_cos, np.ones_like(head_cos)], axis=1),
            np.concatenate([head_sin, np.zeros_like(head_sin)], axis=1),
        ]
    ).astype(np.float32)


def nt(a, b):
    return lax.dot_general(a, b, (((1,), (1,)), ((), ())), preferred_element_type=F32)


def tn(a, b):
    return lax.dot_general(a, b, (((0,), (0,)), ((), ())), preferred_element_type=F32)


def nn(a, b):
    return jnp.dot(a, b, preferred_element_type=F32)


def kernel(
    x_hbm, c_hbm, t_hbm, wq_hbm, wo_hbm, gain_hbm, rope_hbm,
    ug_out, gq_out, go_out, gg_out,
    wq, wo, gain, rope, xg, dyg, norm_rows, n_t, n_tr, gpr, q_rot, kk, vv, prob, att, gn, rsr, way, ug,
    dy_far, att_far, part, part_r, part_way, wq_part, wq_part_r, gain_sum, g1, g2, g3, gq_v, gq_low, go_v, go_far, gg_v,
    w_sem, own_sem, out_sem, ag_s, ag_r, dy_s, dy_r, rs_s, rs_r, sh_s, sh_r,
    nt_s, nt_r, gp_s, gp_r, pair_s, pair_r, po_s, po_r, g1_s, g1_r, g2_s, g2_r,
):
    s, c, j = lax.axis_index("section"), lax.axis_index("tensor"), lax.axis_index("dp")
    n_s, n_c, n_j = DIMS["sections"], DIMS["tensor"], DIMS["dp"]
    rows = x_hbm.shape[1]
    length = rows * n_c
    width = x_hbm.shape[2]
    slice_q = gq_out.shape[1]
    slice_o = go_out.shape[1]
    own = pl.ds(pl.multiple_of(c * rows, rows), rows)
    lane = lax.broadcasted_iota(jnp.int32, (length, 128), 1)
    low_half = (lane % HD) < (HD // 2)
    first_head = lane < HD

    def tensor_peer(k):
        return lax.rem(c + k, n_c)

    z, y = lax.rem(j, 4), lax.div(j, 4)
    far = (1 - y) * 4 + z
    half = width // 2
    half_lanes = pl.ds(pl.multiple_of(y * half, half), half)
    far_lanes = pl.ds(pl.multiple_of((1 - y) * half, half), half)

    def z_peer(k):
        return lax.rem(z + k, 4)

    def at_z(k):
        return (s, c, y * 4 + z_peer(k))

    pair = (s, c, far)
    z_order = (1, 3, 2)

    sent = []

    def send(src, dst, s_sem, r_sem, to):
        copy = pltpu.make_async_remote_copy(
            src_ref=src, dst_ref=dst, send_sem=s_sem, recv_sem=r_sem, device_id=to, device_id_type=MESH
        )
        copy.start()
        sent.append(copy)
        return copy

    loads = {}

    def load(name, src, dst, i):
        loads[name] = pltpu.make_async_copy(src, dst, w_sem.at[i])
        loads[name].start()

    load("gain", gain_hbm, gain, 0)
    load("rope", rope_hbm, rope, 1)
    own_copies = {}
    for i, (name, src, dst) in enumerate(
        [(("x", u), x_hbm.at[u], xg.at[u, own]) for u in range(4)]
        + [(("d", u), c_hbm.at[u], dyg.at[u, own]) for u in range(2)]
    ):
        own_copies[name] = pltpu.make_async_copy(src, dst, own_sem.at[i])
        own_copies[name].start()
    barrier = pltpu.get_barrier_semaphore()
    friends = [(s, tensor_peer(k), j) for k in (1, 2, 3)] + [at_z(k) for k in (1, 2, 3)]
    friends += [pair, (lax.rem(s + 1, n_s), c, j), (lax.rem(s + n_s - 1, n_s), c, j)]
    for friend in friends:
        pl.semaphore_signal(barrier, inc=1, device_id=friend, device_id_type=MESH)
    load("wq1", wq_hbm.at[1], wq.at[1], 2)
    load("wo1", wo_hbm.at[1], wo.at[1], 3)
    load("wq0", wq_hbm.at[0], wq.at[0], 4)
    load("wo0", wo_hbm.at[0], wo.at[0], 5)

    pl.semaphore_wait(barrier, len(friends))

    half_rows = rows // 2
    right, left = (s, tensor_peer(1), j), (s, tensor_peer(3), j)
    gathers = {}
    pair_copies = {}

    def pair_send(name, i, src, dst):
        pair_copies[name] = send(src, dst, pair_s.at[i], pair_r.at[i], pair)

    def share_dy(u, blocks):
        for k in blocks:
            at = pl.ds(pl.multiple_of(tensor_peer(k) * rows, rows), rows)
            src = c_hbm.at[u, :, far_lanes] if u < 2 and k == 0 else dyg.at[u, at, far_lanes]
            pair_send(("dy", u, k), 13 + 4 * u + k, src, dy_far.at[u, at])

    def block_half(block, h):
        return pl.ds(pl.multiple_of(block * rows + h * half_rows, half_rows), half_rows)

    def gather(kind, u):
        x_like = kind == "x"
        buf = xg.at[u] if x_like else dyg.at[u]
        src = x_hbm.at[u] if x_like else c_hbm.at[u] if u < 2 else dyg.at[u, own]
        ss, rs = (ag_s, ag_r) if x_like else (dy_s, dy_r)
        gathers[kind, u] = [
            send(src, buf.at[own], ss.at[u, 0], rs.at[u, 0], right),
            send(src, buf.at[own], ss.at[u, 1], rs.at[u, 1], left),
        ]
        if not x_like:
            share_dy(u, (0,))

    def pass_on(kind, u):
        x_like = kind == "x"
        buf = xg.at[u] if x_like else dyg.at[u]
        ss, rs = (ag_s, ag_r) if x_like else (dy_s, dy_r)
        near = gathers[kind, u]
        near[0].wait_recv()
        first = buf.at[block_half(tensor_peer(3), 0)]
        on = [send(first, first, ss.at[u, 2], rs.at[u, 2], right)]
        near[1].wait_recv()
        second = buf.at[block_half(tensor_peer(1), 1)]
        on.append(send(second, second, ss.at[u, 3], rs.at[u, 3], left))
        gathers[kind, u] = on
        if not x_like:
            share_dy(u, (1, 3))

    def gathered(kind, u):
        if (kind, u) in own_copies:
            own_copies[kind, u].wait()
        for copy in gathers[kind, u]:
            copy.wait_recv()
        if kind == "d":
            share_dy(u, (2,))

    def partner(chunk):
        return jnp.where(low_half, pltpu.roll(chunk, 96, 1), pltpu.roll(chunk, 32, 1))

    def normalize(u):
        m = u % 2
        x = xg[u].astype(F32)
        inverse = lax.rsqrt(jnp.mean(x * x, axis=-1, keepdims=True) + EPSILON)
        normed = (x * inverse * gain[m]).astype(BF16)
        for i in range(width // 256):
            n_t[u, i * 256 : (i + 1) * 256, :] = jnp.transpose(normed[:, i * 256 : (i + 1) * 256])
        norm_rows[u % 2] = normed

    def forward(u):
        t, m = u // 2, u % 2
        projected = nn(norm_rows[u % 2], wq[m])
        for i in range(4):
            chunk = projected[:, i * 128 : (i + 1) * 128]
            q_rot[u, :, i * 128 : (i + 1) * 128] = (chunk * rope[0] + partner(chunk) * rope[1]).astype(BF16)
        chunk = projected[:, 512:640]
        both = (chunk * rope[2] + partner(chunk) * rope[3]).astype(BF16).astype(F32)
        key_low = jnp.where(first_head, both, 0.0)
        value_high = jnp.where(first_head, 0.0, both)
        kk[u, 0:128, :] = key_low.astype(BF16)
        kk[u, 128:256, :] = pltpu.roll(key_low, HD, 1).astype(BF16)
        vv[u, 0:128, :] = pltpu.roll(value_high, HD, 1).astype(BF16)
        vv[u, 128:256, :] = value_high.astype(BF16)
        causal = lax.broadcasted_iota(jnp.int32, (length, length), 0) >= lax.broadcasted_iota(
            jnp.int32, (length, length), 1
        )
        for i in range(4):
            scores = nt(q_rot[u, :, i * 128 : (i + 1) * 128], kk[u]) * SCALE
            low = []
            for h in range(2):
                part_scores = jnp.where(causal, scores[:, h * 128 : (h + 1) * 128], -1e30)
                e = jnp.exp(part_scores - jnp.max(part_scores, axis=-1, keepdims=True))
                p = e / jnp.sum(e, axis=-1, keepdims=True)
                prob[u, :, (2 * i + h) * 128 : (2 * i + h + 1) * 128] = p
                low.append(p.astype(BF16))
            attended = nn(jnp.concatenate(low, axis=1), vv[u]).astype(BF16)
            att[m, i * 128 : (i + 1) * 128, t * 128 : (t + 1) * 128] = jnp.transpose(attended)

    def backward(u):
        t, m = u // 2, u % 2
        grad_att = nt(dyg[u], wo[m]).astype(BF16)
        acc_k = jnp.zeros((256, 128), F32)
        acc_v = jnp.zeros((256, 128), F32)
        slot = pl.ds(pl.multiple_of((z * 2 + t) * 128, 128), 128)
        for i in range(4):
            da = grad_att[:, i * 128 : (i + 1) * 128]
            grad_soft = nt(da, vv[u])
            low, grads = [], []
            for h in range(2):
                p = prob[u, :, (2 * i + h) * 128 : (2 * i + h + 1) * 128]
                g = grad_soft[:, h * 128 : (h + 1) * 128]
                total = jnp.sum(p * g, axis=-1, keepdims=True)
                grads.append((p * (g - total) * SCALE).astype(BF16))
                low.append(p.astype(BF16))
            grads = jnp.concatenate(grads, axis=1)
            low = jnp.concatenate(low, axis=1)
            gq = nn(grads, kk[u])
            gpr[m, slot, i * 128 : (i + 1) * 128] = (gq * rope[0] - partner(gq) * rope[1]).astype(BF16)
            acc_k = acc_k + tn(grads, q_rot[u, :, i * 128 : (i + 1) * 128])
            acc_v = acc_v + tn(low, da)
        grad_k = acc_k[0:128] + pltpu.roll(acc_k[128:256], HD, 1)
        grad_v = pltpu.roll(acc_v[0:128], HD, 1) + acc_v[128:256]
        both = jnp.where(first_head, grad_k, grad_v)
        gpr[m, slot, 512:640] = (both * rope[2] - partner(both) * rope[3]).astype(BF16)
        gp = gpr[m, slot, :]
        for i in range(width // 512):
            gn[u, :, i * 512 : (i + 1) * 512] = nt(gp, wq[m, i * 512 : (i + 1) * 512, :]).astype(BF16)

    scatters = {}

    def scatter(u):
        def out(slot, block, h, to):
            return send(gn.at[u, block_half(block, h)], rsr.at[u, slot], rs_s.at[u, slot], rs_r.at[u, slot], to)

        scatters[u] = {
            0: out(0, tensor_peer(2), 0, right),
            3: out(3, tensor_peer(2), 1, left),
            1: out(1, tensor_peer(1), 1, right),
            4: out(4, tensor_peer(3), 0, left),
        }

    def scatter_on(u):
        for i, slot, block, h, to in ((0, 0, tensor_peer(1), 0, right), (1, 3, tensor_peer(3), 1, left)):
            scatters[u].pop(slot).wait_recv()
            both = gn[u, block_half(block, h), :].astype(F32) + rsr[u, slot].astype(F32)
            way[u, i] = both.astype(BF16)
            scatters[u][2 + 3 * i] = send(
                way.at[u, i], rsr.at[u, 2 + 3 * i], rs_s.at[u, 2 + 3 * i], rs_r.at[u, 2 + 3 * i], to
            )

    def finish(u):
        t, m = u // 2, u % 2
        for copy in scatters[u].values():
            copy.wait_recv()
        total = gn[u, own, :].astype(F32) + jnp.concatenate(
            [
                rsr[u, 2].astype(F32) + rsr[u, 4].astype(F32),
                rsr[u, 1].astype(F32) + rsr[u, 5].astype(F32),
            ],
            axis=0,
        )
        x = xg[u, own, :].astype(F32)
        inverse = lax.rsqrt(jnp.mean(x * x, axis=-1, keepdims=True) + EPSILON)
        unit = x * inverse
        g = total * gain[m]
        result = dyg[u, own, :].astype(F32) + inverse * (g - unit * jnp.mean(g * unit, axis=-1, keepdims=True))
        ug[u] = result.astype(BF16)
        scale = jnp.sum(total * unit, axis=0, keepdims=True)
        if t == 0:
            gain_sum[m] = scale
        else:
            gain_sum[m] = gain_sum[m] + scale

    def shift_copy(m):
        step = 1 if m == 1 else -1
        return pltpu.make_async_remote_copy(
            src_ref=ug.at[m],
            dst_ref=dyg.at[2 + m, own],
            send_sem=sh_s.at[m],
            recv_sem=sh_r.at[m],
            device_id=(lax.rem(s + step + n_s, n_s), c, j),
            device_id_type=MESH,
        )

    def sends(m):
        return s < n_s - 1 if m == 1 else s > 0

    def receives(m):
        return s > 0 if m == 1 else s < n_s - 1

    top_copy = pltpu.make_async_copy(t_hbm, dyg.at[3, own], own_sem.at[6])
    turn_copy = pltpu.make_async_copy(ug.at[1], dyg.at[2, own], own_sem.at[7])

    def shift(m):
        pl.when(sends(m))(lambda: shift_copy(m).start())
        if m == 1:
            pl.when(s == 0)(lambda: top_copy.start())
            pl.when(s == n_s - 1)(lambda: turn_copy.start())

    def shifted(m):
        pl.when(receives(m))(lambda: shift_copy(m).wait_recv())
        pl.when(jnp.logical_not(receives(m)))(lambda: (top_copy if m == 1 else turn_copy).wait())

    normed_copies, grad_copies, part_copies = {}, {}, {}
    own_normed = {}

    def rows_of(block, size):
        return pl.ds(pl.multiple_of(block * size, size), size)

    def spread_normed(u):
        t, m = u // 2, u % 2
        lanes = pl.ds(pl.multiple_of((z * 2 + t) * 128, 128), 128)
        own_normed[u] = []
        normed_copies[u] = []
        for b in range(2):
            copy = pltpu.make_async_copy(
                n_t.at[u, rows_of(b * 4 + z, slice_q)], n_tr.at[m, b, :, lanes], own_sem.at[8 + u * 2 + b]
            )
            copy.start()
            own_normed[u].append(copy)
        for k in z_order:
            for b in range(2):
                normed_copies[u].append(
                    send(
                        n_t.at[u, rows_of(b * 4 + z_peer(k), slice_q)],
                        n_tr.at[m, b, :, lanes],
                        nt_s.at[u, b, k - 1],
                        nt_r.at[u, b, k - 1],
                        at_z(k),
                    )
                )

    def tokens_of(block, t, h=None):
        start = (block * 2 + t) * 128
        if h is None:
            return pl.ds(pl.multiple_of(start, 128), 128)
        return pl.ds(pl.multiple_of(start + h * 64, 64), 64)

    def spread_grad(u):
        t, m = u // 2, u % 2
        mine = gpr.at[m, tokens_of(z, t)]
        grad_copies[u] = [
            send(mine, mine, gp_s.at[u, 0], gp_r.at[u, 0], at_z(1)),
            send(mine, mine, gp_s.at[u, 1], gp_r.at[u, 1], at_z(3)),
        ]

    def spread_grad_on(u):
        t, m = u // 2, u % 2
        near = grad_copies[u]
        near[0].wait_recv()
        first = gpr.at[m, tokens_of(z_peer(3), t, 0)]
        on = [send(first, first, gp_s.at[u, 2], gp_r.at[u, 2], at_z(1))]
        near[1].wait_recv()
        second = gpr.at[m, tokens_of(z_peer(1), t, 1)]
        on.append(send(second, second, gp_s.at[u, 3], gp_r.at[u, 3], at_z(3)))
        grad_copies[u] = on

    def share_attended(u):
        t, m = u // 2, u % 2
        lanes = pl.ds(t * 128, 128)
        pair_send(("att", u), u, att.at[m, :, lanes], att_far.at[m, :, lanes])


    def out_part(m):
        for u in (m, 2 + m):
            pair_copies["att", u].wait_recv()
            for k in range(4):
                pair_copies["dy", u, k].wait_recv()
        lhs = jnp.concatenate([att[m], att_far[m]], axis=1)
        rhs = jnp.concatenate([dyg[m, :, half_lanes], dyg[2 + m, :, half_lanes], dy_far[m], dy_far[2 + m]], axis=0)
        for i in range(half // 256):
            part[m, :, i * 256 : (i + 1) * 256] = nn(lhs, rhs[:, i * 256 : (i + 1) * 256]).astype(BF16)

    def spread_out(m):
        def out(slot, block, b, to):
            src = part.at[m, rows_of(b * 4 + block, slice_o)]
            return send(src, part_r.at[m, slot], po_s.at[m, slot], po_r.at[m, slot], to)

        part_copies[m] = {
            0: out(0, z_peer(2), 0, at_z(1)),
            3: out(3, z_peer(2), 1, at_z(3)),
            1: out(1, z_peer(1), 1, at_z(1)),
            4: out(4, z_peer(3), 0, at_z(3)),
        }

    def spread_out_on(m):
        for i, slot, block, b, to in ((0, 0, z_peer(1), 0, at_z(1)), (1, 3, z_peer(3), 1, at_z(3))):
            part_copies[m].pop(slot).wait_recv()
            both = part[m, rows_of(b * 4 + block, slice_o), :].astype(F32) + part_r[m, slot].astype(F32)
            part_way[m, i] = both.astype(BF16)
            last = 2 + 3 * i
            part_copies[m][last] = send(
                part_way.at[m, i], part_r.at[m, last], po_s.at[m, last], po_r.at[m, last], to
            )

    def out_sum(m):
        for copy in part_copies[m].values():
            copy.wait_recv()
        totals = []
        for b, slots in ((0, (2, 4)), (1, (1, 5))):
            total = part[m, rows_of(b * 4 + z, slice_o), :].astype(F32)
            for slot in slots:
                total = total + part_r[m, slot].astype(F32)
            totals.append(total.astype(BF16))
        go_v[m, :, half_lanes] = jnp.where(y == 0, totals[0], totals[1])
        go_far[m] = jnp.where(y == 0, totals[1], totals[0])
        pair_send(("out", m), 8 + m, go_far.at[m], go_v.at[m, :, half_lanes])

    def qkv_part(m):
        for u in (m, 2 + m):
            for copy in own_normed[u]:
                copy.wait()
            for copy in normed_copies[u] + grad_copies[u]:
                copy.wait_recv()
        wq_part[m] = nn(n_tr[m, 1 - y], gpr[m]).astype(BF16)
        pair_send(("wq", m), 10 + m, wq_part.at[m], wq_part_r.at[m])
        return nn(n_tr[m, y], gpr[m])

    gather("x", 1)
    gather("d", 1)
    pass_on("x", 1)
    gather("x", 0)
    pass_on("d", 1)
    gather("d", 0)

    loads["gain"].wait()
    loads["rope"].wait()
    gathered("x", 1)
    normalize(1)
    spread_normed(1)
    loads["wq1"].wait()
    forward(1)
    share_attended(1)
    pass_on("x", 0)
    gathered("d", 1)
    loads["wo1"].wait()
    backward(1)
    scatter(1)
    spread_grad(1)
    pass_on("d", 0)
    gathered("x", 0)
    normalize(0)
    spread_normed(0)
    scatter_on(1)
    gather("x", 3)
    loads["wq0"].wait()
    forward(0)
    share_attended(0)
    gathered("d", 0)
    loads["wo0"].wait()
    backward(0)
    scatter(0)
    spread_grad_on(1)
    spread_grad(0)
    finish(1)
    shift(1)
    pass_on("x", 3)
    scatter_on(0)
    gather("x", 2)
    gathered("x", 3)
    normalize(3)
    spread_normed(3)
    finish(0)
    shift(0)
    forward(3)
    share_attended(3)
    shifted(1)
    gather("d", 3)
    pass_on("x", 2)
    shifted(0)
    gather("d", 2)
    spread_grad_on(0)
    pass_on("d", 3)
    gathered("x", 2)
    normalize(2)
    spread_normed(2)
    forward(2)
    share_attended(2)
    pass_on("d", 2)
    gathered("d", 3)
    backward(3)
    scatter(3)
    spread_grad(3)
    gathered("d", 2)
    backward(2)
    scatter(2)
    spread_grad(2)
    scatter_on(3)
    spread_grad_on(3)
    scatter_on(2)
    spread_grad_on(2)
    out_part(1)
    spread_out(1)
    out_part(0)
    spread_out(0)
    outs = []

    def put(src, dst, i):
        outs.append(pltpu.make_async_copy(src, dst, out_sem.at[i]))
        outs[-1].start()

    gq_v[1] = qkv_part(1)
    spread_out_on(1)
    gq_v[0] = qkv_part(0)
    spread_out_on(0)
    finish(3)
    finish(2)
    put(ug, ug_out, 0)

    g1[c] = gain_sum[...]
    first = [send(g1.at[c], g1.at[c], g1_s.at[k - 1], g1_r.at[k - 1], (s, tensor_peer(k), j)) for k in (1, 2, 3)]
    for copy in first:
        copy.wait_recv()
    g2[z] = ((g1[0] + g1[1]) + g1[2]) + g1[3]
    second = [send(g2.at[z], g2.at[z], g2_s.at[k - 1], g2_r.at[k - 1], at_z(k)) for k in (1, 2, 3)]
    out_sum(1)
    for copy in second:
        copy.wait_recv()
    g3[y] = ((g2[0] + g2[1]) + g2[2]) + g2[3]
    pair_send("gain", 12, g3.at[y], g3.at[y])
    def put_qkv(m):
        pair_copies["wq", m].wait_recv()
        gq_low[m] = (gq_v[m] + wq_part_r[m].astype(F32)).astype(BF16)
        put(gq_low.at[m], gq_out.at[m], 1 + m)

    put_qkv(1)
    out_sum(0)
    put_qkv(0)
    for m in (1, 0):
        pair_copies["out", m].wait_recv()
        put(go_v.at[m], go_out.at[m], 3 + m)
    pair_copies["gain"].wait_recv()
    gg_v[...] = g3[0] + g3[1]
    put(gg_v, gg_out, 5)

    for m in (0, 1):
        pl.when(sends(m))(lambda m=m: shift_copy(m).wait_send())
    for copy in sent:
        copy.wait_send()
    for copy in outs:
        copy.wait()


def copy_out(*refs):
    n = len(refs) // 3
    srcs, dsts, held, sems = refs[:n], refs[n : 2 * n], refs[2 * n : 3 * n], refs[3 * n]
    inward = [pltpu.make_async_copy(srcs[i], held[i], sems.at[0, i]) for i in range(n)]
    outward = [pltpu.make_async_copy(held[i], dsts[i], sems.at[1, i]) for i in range(n)]
    for copy in inward:
        copy.start()
    for i in range(n):
        inward[i].wait()
        outward[i].start()
    for copy in outward:
        copy.wait()


def local(layer_in, carry_in, top_grad, w_qkv, w_out, gain):
    ticks, members = layer_in.shape[:2]
    rows, width = layer_in.shape[-2:]
    n_c, n_j = DIMS["tensor"], DIMS["dp"]
    length = rows * n_c
    units = ticks * members
    x = layer_in.reshape(units, rows, width)
    carry = carry_in.reshape(members, rows, width)
    top = top_grad.reshape(rows, width)
    wq = w_qkv[:, 0]
    wo = w_out[:, 0]
    cols, heads = wq.shape[2], wo.shape[1]
    slice_q, slice_o = width // n_j, heads // n_j
    tokens = 4 * ticks * length
    hbm = pl.BlockSpec(memory_space=pl.ANY)
    dma = pltpu.SemaphoreType.DMA
    outs = pl.pallas_call(
        kernel,
        out_shape=(
            jax.ShapeDtypeStruct((units, rows, width), BF16),
            jax.ShapeDtypeStruct((members, slice_q, cols), BF16),
            jax.ShapeDtypeStruct((members, slice_o, width), BF16),
            jax.ShapeDtypeStruct((members, 1, width), F32),
        ),
        in_specs=[hbm] * 7,
        out_specs=(hbm,) * 4,
        scratch_shapes=[
            pltpu.VMEM((members, width, cols), BF16),
            pltpu.VMEM((members, heads, width), BF16),
            pltpu.VMEM((members, 1, width), F32),
            pltpu.VMEM((4, length, 128), F32),
            pltpu.VMEM((units, length, width), BF16),
            pltpu.VMEM((units, length, width), BF16),
            pltpu.VMEM((members, length, width), BF16),
            pltpu.VMEM((units, width, length), BF16),
            pltpu.VMEM((members, 2, slice_q, tokens), BF16),
            pltpu.VMEM((members, tokens, cols), BF16),
            pltpu.VMEM((units, length, heads), BF16),
            pltpu.VMEM((units, 256, 128), BF16),
            pltpu.VMEM((units, 256, 128), BF16),
            pltpu.VMEM((units, length, GROUP * 128), F32),
            pltpu.VMEM((members, heads, ticks * length), BF16),
            pltpu.VMEM((units, length, width), BF16),
            pltpu.VMEM((units, 6, rows // 2, width), BF16),
            pltpu.VMEM((units, 2, rows // 2, width), BF16),
            pltpu.VMEM((units, rows, width), BF16),
            pltpu.VMEM((units, length, width // 2), BF16),
            pltpu.VMEM((members, heads, ticks * length), BF16),
            pltpu.VMEM((members, heads, width // 2), BF16),
            pltpu.VMEM((members, 6, slice_o, width // 2), BF16),
            pltpu.VMEM((members, 2, slice_o, width // 2), BF16),
            pltpu.VMEM((members, slice_q, cols), BF16),
            pltpu.VMEM((members, slice_q, cols), BF16),
            pltpu.VMEM((members, 1, width), F32),
            pltpu.VMEM((n_c, members, 1, width), F32),
            pltpu.VMEM((4, members, 1, width), F32),
            pltpu.VMEM((2, members, 1, width), F32),
            pltpu.VMEM((members, slice_q, cols), F32),
            pltpu.VMEM((members, slice_q, cols), BF16),
            pltpu.VMEM((members, slice_o, width), BF16),
            pltpu.VMEM((members, slice_o, width // 2), BF16),
            pltpu.VMEM((members, 1, width), F32),
            dma((6,)), dma((16,)), dma((6,)),
            dma((4, 4)), dma((4, 4)), dma((4, 4)), dma((4, 4)), dma((4, 6)), dma((4, 6)), dma((2,)), dma((2,)),
            dma((4, 2, 3)), dma((4, 2, 3)), dma((4, 4)), dma((4, 4)), dma((29,)), dma((29,)),
            dma((2, 6)), dma((2, 6)), dma((3,)), dma((3,)), dma((3,)), dma((3,)),
        ],
        compiler_params=pltpu.CompilerParams(has_side_effects=True, collective_id=0, vmem_limit_bytes=63 * 1024 * 1024),
    )(x, carry, top, wq, wo, gain, jnp.asarray(rope_tables(length)))
    unit_grads, grad_qkv, grad_out, grad_gain = pl.pallas_call(
        copy_out,
        out_shape=tuple(jax.ShapeDtypeStruct(o.shape, o.dtype) for o in outs),
        in_specs=[hbm] * 4,
        out_specs=(hbm,) * 4,
        scratch_shapes=[pltpu.VMEM(o.shape, o.dtype) for o in outs] + [dma((2, 4))],
    )(*outs)
    return (
        unit_grads.reshape(ticks, members, 1, 1, rows, width),
        grad_qkv[:, None],
        grad_out[:, None],
        grad_gain,
    )


def solution(mesh):
    in_specs = (
        P(None, None, "section", "dp", "tensor", None),
        P(None, "section", "dp", "tensor", None),
        P(None, "dp", "tensor", None),
        P(None, "section", None, "tensor"),
        P(None, "section", "tensor", None),
        P(None, "section", None),
    )
    out_specs = (
        P(None, None, "section", "dp", "tensor", None),
        P(None, "section", "dp", "tensor"),
        P(None, "section", ("tensor", "dp"), None),
        P(None, "section", None),
    )
    return jax.shard_map(local, mesh=mesh, in_specs=in_specs, out_specs=out_specs, check_vma=False)
```
